32 devices in a mesh: role: 2 (over x), gy: 2 (over y), gx: 8 (over z, core).
Axes of the slice: x: 2, y: 2, z: 4, core: 2. Of those that a mesh axis runs over, the one named last changes fastest.
Arguments:
- thermal_anomaly: float32 [16, 192, 2048], P('role', 'gy', 'gx'), may hold values from -6 to 6
- saltiness_anomaly: float32 [16, 192, 2048], P('role', 'gy', 'gx'), may hold values from -6 to 6
- zonal_flow_fraction: bfloat16 [16, 192, 2048], P('role', 'gy', 'gx'), may hold values from -0.5 to 0.5
- meridional_flow_fraction: bfloat16 [16, 192, 2048], P('role', 'gy', 'gx'), may hold values from -0.5 to 0.5
- mixing_coefficient: float32 [16], P('role'), may hold values from 0.03 to 0.2
- continent_patch_numbering: int32 [2], replicated, may hold values from 0 to 15
- parallel_band_coefficients: bfloat16 [16, 4, 12], P('gy'), may hold values from -1.75 to 1.75
- meridian_panel_coefficients: bfloat16 [14, 512, 128], replicated, may hold values from -0.25 to 0.25
- panel_starting_source_meridian: int32 [14], replicated, may hold values from 0 to 1536, as said below
- target_parallel_cluster: int32 [64], replicated, may hold values from 0 to 7, as said below
Outputs:
- remapped: bfloat16 [3, 16, 64, 1792], P(None, 'role', ('gy', 'gx'))
- checksums: float32 [3, 8], replicated
The draws below stay inside these ranges and needn't reach their ends.
Inputs may be any that keep to these rules, and one draw needn't show every extreme that they name: `panel_starting_source_meridian`: every block's window lies within the model grid. `target_parallel_cluster`: each group number names exactly 8 rows.
All inputs are finite; a program needn't handle non-finite values.
Results may differ from the reference program's by a relative error of at most 0.0057.
Values may be sent and summed in bfloat16 or wider, within the bound.
A program may use at most 64 MiB of HBM per device.

```python
import math
import jax
import jax.numpy as jnp
from jax import lax

VERTICAL_LAYERS = 16
CY = 96
CX = 256
TR = 4
SW = 512
TB = 128
MESH_MERID_SIZE = 192
MESH_ZONAL_SIZE = 2048
NTILES = 16
NLAND = 2
NSTRIP = 16
SR = 12
NBLK = 14
NTX = 1792
NTY = 64
NGROUP = 8
N_GY = 2
N_GX = 8


def draw_panel_starting_source_meridian(key, part):
    starts = jax.random.randint(jax.random.fold_in(key, 3), (NBLK,), 0, MESH_ZONAL_SIZE - SW + 1)
    return starts.astype(jnp.int32)


def draw_target_parallel_cluster(key, part):
    order = jax.random.permutation(jax.random.fold_in(key, 7), NTY)
    return (order % NGROUP).astype(jnp.int32)


def steps_of(key, dims, cuts, least, top_value):
    def one(axis_at, parts):
        heights = jax.random.uniform(jax.random.fold_in(jax.random.fold_in(key, 6), axis_at), (parts,), jnp.float32, least / len(cuts), top_value / len(cuts))
        return jnp.repeat(jnp.exp(heights), dims[axis_at] // parts).reshape((-1,) + (1,) * (len(dims) - axis_at - 1))

    level = one(*cuts[0])
    for cut in cuts[1:]:
        level = level * one(*cut)
    return level


def gaussian(key, extent, spread, limit, pieces=(), kind=jnp.bfloat16):
    array = spread * jax.random.normal(key, extent, jnp.float32)
    if pieces:
        array = array * steps_of(key, extent, pieces, -0.22, 0.18)
    return jnp.clip(array, -limit, limit).astype(kind)


def setup_inputs(seed: int = 0) -> dict:
    streams_of = jax.random.split(jax.random.key(seed), 11)
    return {
        "thermal_anomaly": gaussian(streams_of[0], (VERTICAL_LAYERS, MESH_MERID_SIZE, MESH_ZONAL_SIZE), 1.0, 6.0, ((0, 2), (1, 2), (2, 8)), jnp.float32),
        "saltiness_anomaly": gaussian(streams_of[1], (VERTICAL_LAYERS, MESH_MERID_SIZE, MESH_ZONAL_SIZE), 1.0, 6.0, ((0, 2), (1, 2), (2, 8)), jnp.float32),
        "zonal_flow_fraction": jnp.clip(jax.random.uniform(streams_of[2], (VERTICAL_LAYERS, MESH_MERID_SIZE, MESH_ZONAL_SIZE), jnp.float32, -0.5, 0.5) * steps_of(streams_of[2], (VERTICAL_LAYERS, MESH_MERID_SIZE, MESH_ZONAL_SIZE), ((0, 2), (1, 2), (2, 8)), -0.4, 0.0), -0.5, 0.5).astype(jnp.bfloat16),
        "meridional_flow_fraction": jnp.clip(jax.random.uniform(streams_of[3], (VERTICAL_LAYERS, MESH_MERID_SIZE, MESH_ZONAL_SIZE), jnp.float32, -0.5, 0.5) * steps_of(streams_of[3], (VERTICAL_LAYERS, MESH_MERID_SIZE, MESH_ZONAL_SIZE), ((0, 2), (1, 2), (2, 8)), -0.4, 0.0), -0.5, 0.5).astype(jnp.bfloat16),
        "mixing_coefficient": jnp.clip(jnp.exp(math.log(0.2) - 1.89712 * jax.random.uniform(streams_of[4], (VERTICAL_LAYERS,), jnp.float32) ** steps_of(streams_of[4], (VERTICAL_LAYERS,), ((0, 2),), -0.2, 0.2)), 0.03, 0.2),
        "continent_patch_numbering": jax.random.randint(streams_of[5], (NLAND,), 0, NTILES).astype(jnp.int32),
        "parallel_band_coefficients": gaussian(streams_of[6], (NSTRIP, TR, SR), SR ** -0.5, 1.75, ((0, 2),)),
        "meridian_panel_coefficients": gaussian(streams_of[7], (NBLK, SW, TB), SW ** -0.5, 0.25),
        "panel_starting_source_meridian": draw_panel_starting_source_meridian(jax.random.fold_in(streams_of[10], 71), 0),
        "target_parallel_cluster": draw_target_parallel_cluster(jax.random.fold_in(streams_of[10], 71), 0),
    }


def step_level(tracers, east_speed, north_speed, kappa, ocean):
    padded = jnp.pad(tracers, ((0, 0), (1, 1), (0, 0)))
    east = jnp.roll(tracers, -1, axis=2)
    west = jnp.roll(tracers, 1, axis=2)
    north = padded[:, 2:, :]
    south = padded[:, :-2, :]
    tendency = -east_speed * (east - west) * 0.5 - north_speed * (north - south) * 0.5 + kappa * (east + west + north + south - 4.0 * tracers)
    return tracers + ocean * tendency


def density(temp, salt, level):
    return 0.78 * salt - 0.17 * temp * (1.0 + 0.03 * level) - 0.02 * temp * temp


def reference(thermal_anomaly, saltiness_anomaly, zonal_flow_fraction, meridional_flow_fraction, mixing_coefficient, continent_patch_numbering, parallel_band_coefficients, meridian_panel_coefficients, panel_starting_source_meridian, target_parallel_cluster):
    tiles = N_GY * N_GX
    listed = jnp.any(continent_patch_numbering[:, None] == jnp.arange(tiles, dtype=jnp.int32)[None, :], axis=0)
    flags = 1.0 - listed.astype(jnp.float32)
    ocean = jnp.repeat(jnp.repeat(flags.reshape(N_GY, N_GX), CY, axis=0), CX, axis=1)
    lat_f = parallel_band_coefficients.astype(jnp.float32)
    lon_f = meridian_panel_coefficients.astype(jnp.float32)
    vertical_layer_total = jnp.arange(VERTICAL_LAYERS, dtype=jnp.float32)

    def lone_vertical_layer(packed):
        temp, salt, east_raw, north_raw, kappa, level = packed
        east_speed = east_raw.astype(jnp.float32)
        north_speed = north_raw.astype(jnp.float32)
        scalar_field_pair = jnp.stack([temp, salt])
        means = jnp.zeros((3, MESH_MERID_SIZE, MESH_ZONAL_SIZE), jnp.float32)
        for step in range(2):
            scalar_field_pair = step_level(scalar_field_pair, east_speed, north_speed, kappa, ocean)
            rho = density(scalar_field_pair[0], scalar_field_pair[1], level)
            means = means + jnp.stack([scalar_field_pair[0], scalar_field_pair[1], rho])
        means = (0.5 * means).astype(jnp.bfloat16)
        strips = means.astype(jnp.float32).reshape(3, NSTRIP, SR, MESH_ZONAL_SIZE)
        lat_out = jnp.einsum("gts,fgsx->fgtx", lat_f, strips, precision=lax.Precision.HIGHEST)
        lat_out = lat_out.astype(jnp.bfloat16).reshape(3, NTY, MESH_ZONAL_SIZE)

        def block(index):
            window = lax.dynamic_slice_in_dim(lat_out, panel_starting_source_meridian[index].astype(jnp.int32), SW, axis=2)
            return jnp.einsum("frs,st->frt", window.astype(jnp.float32), lon_f[index], precision=lax.Precision.HIGHEST)

        blocks = lax.map(block, jnp.arange(NBLK, dtype=jnp.int32))
        values = jnp.transpose(blocks, (1, 2, 0, 3)).reshape(3, NTY, NBLK * TB)
        quadratic_entries = jnp.sum(values * values, axis=2)
        return values.astype(jnp.bfloat16), quadratic_entries

    regridded_target_field, quadratic_entries = lax.map(lone_vertical_layer, (thermal_anomaly, saltiness_anomaly, zonal_flow_fraction, meridional_flow_fraction, mixing_coefficient, vertical_layer_total))
    remapped = jnp.transpose(regridded_target_field, (1, 0, 2, 3))
    thick = 1.0 + 0.25 * vertical_layer_total
    rows = jnp.arange(NTY, dtype=jnp.float32)
    area = jnp.cos((-75.0 + 150.0 * (rows + 0.5) / NTY) * (math.pi / 180.0))
    weighted = jnp.sum(quadratic_entries * thick[:, None, None], axis=0) * area[None, :]
    onehot = (target_parallel_cluster[:, None] == jnp.arange(NGROUP, dtype=jnp.int32)[None, :]).astype(jnp.float32)
    numer = jnp.dot(weighted, onehot, precision=lax.Precision.HIGHEST)
    denom = jnp.sum(thick) * NTX * jnp.dot(area, onehot, precision=lax.Precision.HIGHEST)
    return remapped, numer / denom[None, :]
```

```python
import functools
import math

import jax
import jax.numpy as jnp
import numpy as np
from jax import lax
from jax.experimental import pallas as pl
from jax.experimental.pallas import tpu as pltpu
from jax.sharding import PartitionSpec as P

LANES = 128
SUB = 8
EDGE = 4
F32 = jnp.float32
BF16 = jnp.bfloat16
MESH = pl.DeviceIdType.MESH


def wrap(value, count):
    return jnp.where(value >= count, value - count, value)


def iota(shape, dim):
    return lax.broadcasted_iota(jnp.int32, shape, dim)


def turn(value, shift, axis):
    size = value.shape[axis]
    shift = shift % size
    return pltpu.roll(value, shift, axis) if shift else value


def position():
    return tuple(lax.axis_index(a) for a in ("role", "gy", "gx"))


def peer_of(dims, d):
    n_role, n_gy, n_gx = dims[:3]
    role, gy, gx = position()
    dx, dyr = d % n_gx, d // n_gx
    dy, dr = dyr % n_gy, dyr // n_gy
    return (wrap(role + dr, n_role), wrap(gy + dy, n_gy), wrap(gx + dx, n_gx))


def kernel(
    dims,
    temp_hbm,
    salt_hbm,
    zonal_hbm,
    merid_hbm,
    panel_hbm,
    kappa_ref,
    land_ref,
    start_ref,
    cluster_ref,
    area_ref,
    band_ref,
    out_hbm,
    sums_ref,
    x0,
    x1,
    uv,
    means,
    halo_x,
    halo_uv,
    cols,
    band_rows,
    lat_send,
    lat,
    e_send,
    e_recv,
    placed,
    panel,
    shifted,
    result,
    out_vmem,
    gather,
    in_sems,
    panel_sems,
    halo_send_sems,
    halo_recv_sems,
    a2a_send_sems,
    a2a_recv_sems,
    local_sems,
    e_send_sems,
    e_recv_sems,
    sum_sems,
    out_sem,
):
    n_role, n_gy, n_gx, levels, cy, cx, trows, srows, nblk, sw, tb, groups = dims
    role, gy, gx = position()
    total = n_role * n_gy * n_gx
    me = (role * n_gy + gy) * n_gx + gx
    lev_grp = 16 // trows
    halves = levels // lev_grp
    lev_rows = lev_grp * trows
    half_rows = 3 * lev_rows
    nk = EDGE * levels
    peer = functools.partial(peer_of, dims)

    sources = ((temp_hbm, x0.at[0]), (salt_hbm, x0.at[1]), (zonal_hbm, uv.at[0]), (merid_hbm, uv.at[1]))
    loads = [pltpu.make_async_copy(src, dst, in_sems.at[i]) for i, (src, dst) in enumerate(sources)]
    for load in loads:
        load.start()
    panel_loads = [
        pltpu.make_async_copy(panel_hbm.at[j], panel.at[j], panel_sems.at[j]) for j in range(nblk)
    ]
    for load in panel_loads:
        load.start()

    barrier = pltpu.get_barrier_semaphore()
    greeted = set(range(1, n_gx)) | {d * n_gx for d in range(1, n_role * n_gy)}
    for dy in {1, n_gy - 1}:
        for dx in {1, n_gx - 1}:
            greeted.add(dy * n_gx + dx)
    greeted = sorted(greeted)
    for d in greeted:
        pl.semaphore_signal(barrier, inc=1, device_id=peer(d), device_id_type=MESH)

    has_below = gy > 0
    has_above = gy < n_gy - 1

    @pl.when(gy == 0)
    def _():
        halo_x[0] = jnp.zeros_like(halo_x[0])
        halo_uv[0] = jnp.zeros_like(halo_uv[0])
        for i in range(4):
            cols[i, pl.ds(0, SUB)] = jnp.zeros((SUB, LANES), F32)

    @pl.when(gy == n_gy - 1)
    def _():
        halo_x[1] = jnp.zeros_like(halo_x[1])
        halo_uv[1] = jnp.zeros_like(halo_uv[1])
        for i in range(4):
            cols[i, pl.ds(SUB + cy, SUB)] = jnp.zeros((SUB, LANES), F32)

    columns = n_gx * cx
    lat[columns // LANES] = jnp.zeros((halves * half_rows, LANES), BF16)

    def ocean_of(dy, dx):
        ty = gy + dy
        tx = wrap(gx + dx + n_gx, n_gx)
        number = jnp.full((1, cx), ty * n_gx + tx, jnp.int32)
        flag = jnp.where((jnp.full((1, cx), ty, jnp.int32) >= 0) & (jnp.full((1, cx), ty, jnp.int32) < n_gy), 1.0, 0.0)
        for i in range(land_ref.shape[0]):
            flag = jnp.where(jnp.full((1, cx), land_ref[i], jnp.int32) == number, 0.0, flag)
        return flag

    ocean = ocean_of(0, 0)

    band_rows[...] = jnp.zeros_like(band_rows)
    for g in range(n_gx):
        band_rows[pl.ds(g * trows, trows), pl.ds(0, srows)] = band_ref[g].astype(F32)
    brows = band_rows.shape[0]
    out_r, in_r = n_gx * lev_rows, lev_grp * cy
    flat = band_rows[...].astype(BF16)
    ri, rq = iota((out_r, brows), 0), iota((out_r, brows), 1)
    pick_r = (lax.div(ri, lev_rows) == lax.div(rq, trows)) & (
        lax.rem(ri, trows) == lax.rem(rq, trows)
    )
    spread = jnp.dot(pick_r.astype(F32).astype(BF16), flat, preferred_element_type=F32)
    cs, cc = iota((LANES, in_r), 0), iota((LANES, in_r), 1)
    pick_c = (lax.rem(lax.rem(cc, cy), srows) == cs).astype(F32).astype(BF16)
    spread = jnp.dot(spread.astype(BF16), pick_c, preferred_element_type=F32)
    ai, ac = iota((out_r, in_r), 0), iota((out_r, in_r), 1)
    keep = (lax.div(lax.rem(ai, lev_rows), trows) == lax.div(ac, cy)) & (
        lax.div(lax.rem(ac, cy), srows) == lax.div(ai, lev_rows)
    )
    band = jnp.where(keep, spread, 0.0).astype(BF16)

    lane = iota((1, LANES), 1)
    quad = lax.div(lane, EDGE)
    col = lax.rem(lane, EDGE)

    for load in loads:
        load.wait()
    first = jnp.zeros((cy, LANES), F32)
    last = jnp.zeros((cy, LANES), F32)
    for q in range(4 * levels):
        kind, l = q // levels, q % levels
        source = x0.at[kind, l] if kind < 2 else uv.at[kind - 2, l]
        head = source[:, pl.ds(0, LANES)].astype(F32)
        tail = source[:, pl.ds(cx - LANES, LANES)].astype(F32)
        first = jnp.where(quad == q, turn(head, EDGE * q, 1), first)
        last = jnp.where(quad == q, turn(tail, EDGE * (q + 1), 1), last)
    cols[1, pl.ds(SUB, cy)] = first
    cols[2, pl.ds(SUB, cy)] = last

    west = wrap(gx + n_gx - 1, n_gx)
    east = wrap(gx + 1, n_gx)
    own_w, own_e = cols.at[1, pl.ds(SUB, cy)], cols.at[2, pl.ds(SUB, cy)]
    plan = [
        (None, None, own_w, cols.at[3, pl.ds(SUB, cy)], (role, gy, west)),
        (None, None, own_e, cols.at[0, pl.ds(SUB, cy)], (role, gy, east)),
    ]
    for side, (can_send, can_recv) in enumerate(((has_below, has_above), (has_above, has_below))):
        ty = gy - 1 if side == 0 else gy + 1
        mine = SUB if side == 0 else cy
        theirs = SUB + cy if side == 0 else 0
        for block, there, tx in ((1, 1, gx), (2, 2, gx), (1, 3, west), (2, 0, east)):
            plan.append(
                (
                    can_send,
                    can_recv,
                    cols.at[block, pl.ds(mine, SUB)],
                    cols.at[there, pl.ds(theirs, SUB)],
                    (role, ty, tx),
                )
            )
        row = 0 if side == 0 else cy - 2
        slot = 0 if side == 0 else SUB - 2
        for t, ref in enumerate((temp_hbm, salt_hbm)):
            plan.append(
                (
                    can_send,
                    can_recv,
                    ref.at[:, pl.ds(row, 2), :],
                    halo_x.at[1 - side, t, :, pl.ds(slot, 2), :],
                    (role, ty, gx),
                )
            )
        row = 0 if side == 0 else cy - SUB
        for t, ref in enumerate((zonal_hbm, merid_hbm)):
            plan.append(
                (
                    can_send,
                    can_recv,
                    ref.at[:, pl.ds(row, SUB), :],
                    halo_uv.at[1 - side, t],
                    (role, ty, gx),
                )
            )

    def when(cond, do):
        if cond is None:
            do()
        else:
            pl.when(cond)(do)

    halos = []
    for i, (can_send, can_recv, src, dst, target) in enumerate(plan):
        copy = pltpu.make_async_remote_copy(
            src_ref=src,
            dst_ref=dst,
            send_sem=halo_send_sems.at[i],
            recv_sem=halo_recv_sems.at[i],
            device_id=target,
            device_id_type=MESH,
        )
        halos.append((can_send, can_recv, copy))
    column_halos = halos[:2] + halos[2:6] + halos[10:14]
    row_halos = halos[6:10] + halos[14:18]

    pl.semaphore_wait(barrier, len(greeted))
    for can_send, _, copy in halos:
        when(can_send, copy.start)

    level0 = role * levels

    def advance(c, e, w, n, b, u, v, kap):
        return (1.0 - 4.0 * kap) * c + (kap * (e + w + n + b) - u * (e - w) - v * (n - b))

    def whole(c, u, v, kap):
        return advance(
            c, turn(c, -1, 1), turn(c, 1, 1), turn(c, -1, 0), turn(c, 1, 0), u, v, kap
        )

    def density(temp, salt, factor):
        return 0.78 * salt - factor * temp - 0.02 * temp * temp

    def factor_of(l):
        return 0.17 * (1.0 + 0.03 * (level0 + l).astype(F32))

    wide = iota((1, cx), 1)
    at_edge = (wide < 2) | (wide >= cx - 2)
    tiles = cx // LANES
    order = sorted(range(1, n_gx), key=lambda d: -min(d, n_gx - d))
    at_end = (gx == 0) | (gx == n_gx - 1)

    def bulk(h, d):
        target = wrap(gx + d, n_gx)
        return target, pltpu.make_async_remote_copy(
            src_ref=lat_send.at[h, target],
            dst_ref=lat.at[pl.ds(gx * tiles, tiles), pl.ds(h * half_rows, half_rows)],
            send_sem=a2a_send_sems.at[h, d],
            recv_sem=a2a_recv_sems.at[h, d],
            device_id=(role, gy, target),
            device_id_type=MESH,
        )

    def local(h):
        return pltpu.make_async_copy(
            lat_send.at[h, gx],
            lat.at[pl.ds(gx * tiles, tiles), pl.ds(h * half_rows, half_rows)],
            local_sems.at[h],
        )

    def stage(h, g, f, rows):
        for i in range(tiles):
            lat_send[h, g, i, pl.ds(f * lev_rows, lev_rows)] = rows[
                :, i * LANES : (i + 1) * LANES
            ]

    for h in range(halves):
        for l in range(h * lev_grp, (h + 1) * lev_grp):
            u = uv[0, l].astype(F32) * (0.5 * ocean)
            v = uv[1, l].astype(F32) * (0.5 * ocean)
            kap = kappa_ref[l] * ocean
            one = [whole(x0[t, l], u, v, kap) for t in range(2)]
            two = [whole(one[t], u, v, kap) for t in range(2)]
            factor = factor_of(l)
            r1 = density(one[0], one[1], factor)
            r2 = density(two[0], two[1], factor)
            x1[0, l] = one[0]
            x1[1, l] = one[1]
            means[0, l] = (0.5 * (one[0] + two[0])).astype(BF16)
            means[1, l] = (0.5 * (one[1] + two[1])).astype(BF16)
            means[2, l] = (0.5 * (r1 + r2)).astype(BF16)
        for f in range(3):
            rows = means[f, pl.ds(h * lev_grp, lev_grp)].reshape(in_r, cx)
            got = jnp.dot(
                band[lev_rows : out_r - lev_rows], rows, preferred_element_type=F32
            )
            got = jnp.where(at_edge, 0.0, got).astype(BF16)
            for g in range(1, n_gx - 1):
                stage(h, g, f, got[(g - 1) * lev_rows : g * lev_rows])
        for d in order:
            target, copy = bulk(h, d)
            pl.when((target > 0) & (target < n_gx - 1))(copy.start)
        pl.when(jnp.logical_not(at_end))(local(h).start)

    for _, can_recv, copy in column_halos:
        when(can_recv, copy.wait_recv)
    cye = cy + 2 * SUB
    row_e = iota((cye, 1), 0)
    kap_l = jnp.zeros((1, LANES), F32)
    factor_l = jnp.zeros((1, LANES), F32)
    lane_level = lax.div(lax.rem(lane, nk), EDGE)
    for l in range(levels):
        kap_l = jnp.where(lane_level == l, kappa_ref[l], kap_l)
        factor_l = jnp.where(lane_level == l, factor_of(l), factor_l)

    flags = {(dy, dx): ocean_of(dy, dx)[:, :LANES] for dy in (-1, 0, 1) for dx in (-1, 0, 1)}

    def coefficients(i, dx):
        block = cols[i]
        oc = jnp.where(
            row_e < SUB, flags[-1, dx], jnp.where(row_e < SUB + cy, flags[0, dx], flags[1, dx])
        )
        half = 0.5 * oc
        u = jnp.where(lane < nk, turn(block, -2 * nk, 1), turn(block, -nk, 1)) * half
        v = jnp.where(lane < nk, turn(block, -3 * nk, 1), turn(block, -2 * nk, 1)) * half
        return u, v, kap_l * oc

    def step_left(left, right, coef):
        e = jnp.where(col == EDGE - 1, turn(right, EDGE - 1, 1), turn(left, -1, 1))
        return advance(left, e, turn(left, 1, 1), turn(left, -1, 0), turn(left, 1, 0), *coef)

    def step_right(left, right, coef):
        w = jnp.where(col == 0, turn(left, 1 - EDGE, 1), turn(right, 1, 1))
        return advance(
            right, turn(right, -1, 1), w, turn(right, -1, 0), turn(right, 1, 0), *coef
        )

    own = coefficients(1, 0)
    left1 = step_left(cols[0], cols[1], coefficients(0, -1))
    west1 = step_right(cols[0], cols[1], own)
    west2 = step_right(left1, west1, own)
    own = coefficients(2, 0)
    east1 = step_left(cols[2], cols[3], own)
    right1 = step_right(cols[2], cols[3], coefficients(3, 1))
    east2 = step_left(east1, right1, own)
    both1 = jnp.where(col < 2, west1, east1)[SUB : SUB + cy]
    both2 = jnp.where(col < 2, west2, east2)[SUB : SUB + cy]
    rho = 0.5 * (
        density(both1, turn(both1, -nk, 1), factor_l)
        + density(both2, turn(both2, -nk, 1), factor_l)
    )
    packed = jnp.where(
        lane < 2 * nk,
        0.5 * (both1 + both2),
        jnp.where(lane < 3 * nk, turn(rho, 2 * nk, 1), 0.0),
    ).astype(BF16)
    narrow = n_gx * trows
    thin = jnp.dot(flat[:narrow], pick_c[:, :cy], preferred_element_type=F32)
    ei, ec = iota((narrow, cy), 0), iota((narrow, cy), 1)
    thin = jnp.where(lax.div(ec, srows) == lax.div(ei, trows), thin, 0.0).astype(BF16)
    edge_lat = jnp.dot(thin, packed, preferred_element_type=F32).astype(BF16)
    for g in range(n_gx):
        e_send[g] = edge_lat[g * trows : (g + 1) * trows]

    e_copies = []
    for d in order:
        target = wrap(gx + d, n_gx)
        copy = pltpu.make_async_remote_copy(
            src_ref=e_send.at[target],
            dst_ref=e_recv.at[gx],
            send_sem=e_send_sems.at[d],
            recv_sem=e_recv_sems.at[d],
            device_id=(role, gy, target),
            device_id_type=MESH,
        )
        copy.start()
        e_copies.append(copy)
    e_recv[pl.ds(gx, 1)] = e_send[pl.ds(gx, 1)]

    for _, can_recv, copy in row_halos:
        when(can_recv, copy.wait_recv)
    sub8 = iota((SUB, 1), 0)
    ocean_below, ocean_above = ocean_of(-1, 0), ocean_of(1, 0)

    def up(a, b):
        return jnp.where(sub8 == SUB - 1, turn(b, -1, 0), turn(a, -1, 0))

    def down(a, b):
        return jnp.where(sub8 == 0, turn(a, 1, 0), turn(b, 1, 0))

    def rows_step(c, n, b, u, v, kap):
        return advance(c, turn(c, -1, 1), turn(c, 1, 1), n, b, u, v, kap)

    for l in range(levels):
        kap = kappa_ref[l] * ocean
        factor = factor_of(l)
        flow = [uv[i, l, pl.ds(0, 16)].astype(F32)[:SUB] * (0.5 * ocean) for i in range(2)]
        other = [halo_uv[0, i, l].astype(F32) * (0.5 * ocean_below) for i in range(2)]
        kap_o = kappa_ref[l] * ocean_below
        ones, twos = [], []
        for t in range(2):
            far, edge, near = halo_x[0, t, l], x0[t, l, pl.ds(0, SUB)], x0[t, l, pl.ds(SUB, SUB)]
            out1 = rows_step(far, up(far, edge), turn(far, 1, 0), *other, kap_o)
            in1 = rows_step(edge, up(edge, near), down(far, edge), *flow, kap)
            ones.append(in1)
            next1 = x1[t, l, pl.ds(SUB, SUB)]
            twos.append(rows_step(in1, up(in1, next1), down(out1, in1), *flow, kap))
        r = density(*ones, factor) + density(*twos, factor)
        for f, value in enumerate((ones[0] + twos[0], ones[1] + twos[1], r)):
            means[f, l, pl.ds(0, SUB)] = (0.5 * value).astype(BF16)

        flow = [uv[i, l, pl.ds(cy - 16, 16)].astype(F32)[SUB:] * (0.5 * ocean) for i in range(2)]
        other = [halo_uv[1, i, l].astype(F32) * (0.5 * ocean_above) for i in range(2)]
        kap_o = kappa_ref[l] * ocean_above
        ones, twos = [], []
        for t in range(2):
            far = halo_x[1, t, l]
            edge = x0[t, l, pl.ds(cy - SUB, SUB)]
            near = x0[t, l, pl.ds(cy - 2 * SUB, SUB)]
            out1 = rows_step(far, turn(far, -1, 0), down(edge, far), *other, kap_o)
            in1 = rows_step(edge, up(edge, far), down(near, edge), *flow, kap)
            ones.append(in1)
            next1 = x1[t, l, pl.ds(cy - 2 * SUB, SUB)]
            twos.append(rows_step(in1, up(in1, out1), down(next1, in1), *flow, kap))
        r = density(*ones, factor) + density(*twos, factor)
        for f, value in enumerate((ones[0] + twos[0], ones[1] + twos[1], r)):
            means[f, l, pl.ds(cy - SUB, SUB)] = (0.5 * value).astype(BF16)

    ends = jnp.concatenate([band[:lev_rows], band[out_r - lev_rows :]], axis=0)
    for h in range(halves):
        for f in range(3):
            rows = means[f, pl.ds(h * lev_grp, lev_grp)].reshape(in_r, cx)
            got = jnp.dot(ends, rows, preferred_element_type=F32)
            got = jnp.where(at_edge, 0.0, got).astype(BF16)
            stage(h, 0, f, got[:lev_rows])
            stage(h, n_gx - 1, f, got[lev_rows:])
        for d in order:
            target, copy = bulk(h, d)
            pl.when((target == 0) | (target == n_gx - 1))(copy.start)
        pl.when(at_end)(local(h).start)

    depth = sw + LANES
    sub = iota((1, SUB, 1), 1)

    def tile_of(j):
        return lax.div(start_ref[j], LANES)

    blank = jnp.zeros((SUB, tb), F32)
    for j in range(nblk):
        panel_loads[j].wait()
        off = jnp.full((1, tb), start_ref[j] - tile_of(j) * LANES, jnp.int32)
        rows = panel[j].astype(F32)
        parts = [rows[i * SUB : (i + 1) * SUB] for i in range(sw // SUB)]
        bit = 1
        while bit < SUB:
            taken = lax.rem(lax.div(off, bit), 2) == 1
            low = sub8 < bit
            ring = [turn(part, bit, 0) for part in parts] + [blank]
            parts = [
                jnp.where(
                    taken,
                    jnp.where(low, ring[i - 1] if i else blank, ring[i]),
                    parts[i] if i < len(parts) else blank,
                )
                for i in range(len(ring))
            ] if bit == 1 else [
                jnp.where(taken, jnp.where(low, ring[i - 1] if i else blank, ring[i]), parts[i])
                for i in range(len(parts))
            ]
            bit *= 2
        step = 1
        while step * SUB < LANES:
            taken = lax.rem(lax.div(off, step * SUB), 2) == 1
            longer = len(parts) + step
            parts = [
                jnp.where(
                    taken,
                    parts[i - step] if i >= step else blank,
                    parts[i] if i < len(parts) else blank,
                )
                for i in range(longer)
            ]
            step *= 2
        assert len(parts) == depth // SUB
        shifted[j] = jnp.concatenate(parts, axis=0).astype(BF16)

    glanes = gather.shape[2]
    lanes = iota((1, glanes), 1)
    labels = lax.rem(lanes, groups)

    def add_area(r, so_far):
        return so_far + jnp.where(labels == cluster_ref[r], area_ref[r], 0.0)

    area_sum = lax.fori_loop(
        0, cluster_ref.shape[0], add_area, jnp.zeros((1, glanes), F32), unroll=8
    )
    thick_total = sum(1.0 + 0.25 * k for k in range(levels * n_role))
    denom = area_sum * (thick_total * nblk * tb)
    first_row = (gy * n_gx + gx) * trows
    out_rows = halves * half_rows
    orow = iota((out_rows, 1), 0)
    ti = lax.rem(orow, trows)
    hot = jnp.zeros((out_rows, glanes), F32)
    for t in range(trows):
        row_hot = jnp.where(labels == cluster_ref[first_row + t], area_ref[first_row + t], 0.0)
        hot = jnp.where(ti == t, row_hot, hot)
    olevel = lax.div(orow, half_rows) * lev_grp + lax.div(lax.rem(orow, lev_rows), trows)
    ofield = lax.div(lax.rem(orow, half_rows), lev_rows)
    thick = 1.0 + 0.25 * (level0 + olevel).astype(F32)
    field = lax.div(lanes, groups)
    hot = jnp.where(ofield == field, hot * thick, 0.0)

    pk, pc = iota((LANES, cx), 0), iota((LANES, cx), 1)
    place = jnp.where(pc < 2, pc, jnp.where(pc >= cx - 2, pc - (cx - EDGE), -1))
    place = (place == lax.rem(pk, EDGE)).astype(F32).astype(BF16)
    mine_q = ofield * levels + olevel
    for copy in e_copies:
        copy.wait_recv()
    for s in range(n_gx):
        block = e_recv[s].astype(F32)
        tall = jnp.concatenate([block] * (out_rows // trows), axis=0)
        tall = jnp.where(quad == mine_q, tall, 0.0).astype(BF16)
        put = jnp.dot(tall, place, preferred_element_type=F32).astype(BF16)
        for i in range(tiles):
            placed[s * tiles + i] = put[:, i * LANES : (i + 1) * LANES]

    for h in range(halves):
        for d in order:
            bulk(h, d)[1].wait_recv()
        local(h).wait()
    for i in range(n_gx * tiles):
        lat[i] = lat[i] + placed[i]
    squares = jnp.zeros((out_rows, tb), F32)
    for j in range(nblk):
        tile = tile_of(j)
        window = jnp.concatenate([lat[tile + i] for i in range(depth // LANES)], axis=1)
        values = jnp.dot(window, shifted[j], preferred_element_type=F32)
        squares = squares + values * values
        result[:, pl.ds(j * tb, tb)] = values
    weighted = jnp.sum(squares, axis=1, keepdims=True) * hot
    part = jnp.sum(weighted, axis=0, keepdims=True) / denom

    def for_others(do):
        if total <= 64:
            for d in range(1, total):
                do(peer(d))
        else:

            @pl.loop(1, total)
            def _(d):
                do(peer(d))

    def send(device):
        pltpu.make_async_remote_copy(
            src_ref=gather.at[me],
            dst_ref=gather.at[me],
            send_sem=sum_sems.at[0],
            recv_sem=sum_sems.at[1],
            device_id=device,
            device_id_type=MESH,
        ).start()

    gather[me] = part
    for_others(send)

    for h in range(halves):
        for f in range(3):
            for i in range(lev_grp):
                row = h * half_rows + f * lev_rows + i * trows
                out_vmem[f, h * lev_grp + i] = result[pl.ds(row, trows), :].astype(BF16)
    store = pltpu.make_async_copy(out_vmem, out_hbm, out_sem)
    store.start()

    for can_send, _, copy in halos:
        when(can_send, copy.wait_send)
    for h in range(halves):
        for d in order:
            bulk(h, d)[1].wait_send()
    for copy in e_copies:
        copy.wait_send()
    store.wait()
    every = gather.at[pl.ds(0, total - 1)]
    for i in (1, 0):
        pltpu.make_async_copy(every, every, sum_sems.at[i]).wait()
    sums = jnp.sum(gather[...], axis=0)
    for f in range(3):
        sums_ref[pl.ds(f, 1), :] = turn(sums, -f * groups, 1)[:, :groups]


def body(
    dims,
    area,
    thermal_anomaly,
    saltiness_anomaly,
    zonal_flow_fraction,
    meridional_flow_fraction,
    mixing_coefficient,
    continent_patch_numbering,
    parallel_band_coefficients,
    meridian_panel_coefficients,
    panel_starting_source_meridian,
    target_parallel_cluster,
):
    n_role, n_gy, n_gx, levels, cy, cx, trows, srows, nblk, sw, tb, groups = dims
    total = n_role * n_gy * n_gx
    lev_grp = 16 // trows
    halves = levels // lev_grp
    half_rows = 3 * lev_grp * trows
    glanes = -(-3 * groups // LANES) * LANES
    hbm = pl.BlockSpec(memory_space=pl.ANY)
    smem = pl.BlockSpec(memory_space=pltpu.SMEM)
    vmem = pl.BlockSpec(memory_space=pltpu.VMEM)
    brows = -(-n_gx * trows // LANES) * LANES
    dma = pltpu.SemaphoreType.DMA
    columns = n_gx * cx
    out_rows = halves * half_rows
    return pl.pallas_call(
        functools.partial(kernel, dims),
        out_shape=(
            jax.ShapeDtypeStruct((3, levels, trows, nblk * tb), BF16),
            jax.ShapeDtypeStruct((3, groups), F32),
        ),
        in_specs=[hbm] * 5 + [smem] * 5 + [vmem],
        out_specs=(hbm, vmem),
        scratch_shapes=[
            pltpu.VMEM((2, levels, cy, cx), F32),
            pltpu.VMEM((2, levels, cy, cx), F32),
            pltpu.VMEM((2, levels, cy, cx), BF16),
            pltpu.VMEM((3, levels, cy, cx), BF16),
            pltpu.VMEM((2, 2, levels, SUB, cx), F32),
            pltpu.VMEM((2, 2, levels, SUB, cx), BF16),
            pltpu.VMEM((4, cy + 2 * SUB, LANES), F32),
            pltpu.VMEM((brows, LANES), F32),
            pltpu.VMEM((halves, n_gx, cx // LANES, half_rows, LANES), BF16),
            pltpu.VMEM((columns // LANES + 1, out_rows, LANES), BF16),
            pltpu.VMEM((n_gx, trows, LANES), BF16),
            pltpu.VMEM((n_gx, trows, LANES), BF16),
            pltpu.VMEM((columns // LANES, out_rows, LANES), BF16),
            pltpu.VMEM((nblk, sw, tb), BF16),
            pltpu.VMEM((nblk, sw + LANES, tb), BF16),
            pltpu.VMEM((out_rows, nblk * tb), F32),
            pltpu.VMEM((3, levels, trows, nblk * tb), BF16),
            pltpu.VMEM((total, 1, glanes), F32),
            dma((4,)),
            dma((nblk,)),
            dma((18,)),
            dma((18,)),
            dma((halves, n_gx)),
            dma((halves, n_gx)),
            dma((halves,)),
            dma((n_gx,)),
            dma((n_gx,)),
            dma((2,)),
            dma(()),
        ],
        compiler_params=pltpu.CompilerParams(
            collective_id=0, has_side_effects=True, vmem_limit_bytes=60 * 1024 * 1024
        ),
        name="ocean",
    )(
        thermal_anomaly,
        saltiness_anomaly,
        zonal_flow_fraction,
        meridional_flow_fraction,
        meridian_panel_coefficients,
        mixing_coefficient,
        continent_patch_numbering,
        panel_starting_source_meridian,
        target_parallel_cluster,
        jnp.asarray(area),
        parallel_band_coefficients,
    )


def solution(mesh):
    in_specs = (
        P("role", "gy", "gx"),
        P("role", "gy", "gx"),
        P("role", "gy", "gx"),
        P("role", "gy", "gx"),
        P("role"),
        P(),
        P("gy", None, None),
        P(),
        P(),
        P(),
    )
    out_specs = (P(None, "role", ("gy", "gx"), None), P())

    def run(*args):
        n_role, n_gy, n_gx = (mesh.shape[a] for a in ("role", "gy", "gx"))
        levels, rows, cols = args[0].shape
        _, trows, srows = args[6].shape
        nblk, sw, tb = args[7].shape
        dims = (
            n_role,
            n_gy,
            n_gx,
            levels // n_role,
            rows // n_gy,
            cols // n_gx,
            trows,
            srows,
            nblk,
            sw,
            tb,
            4 * n_gy,
        )
        nrows = args[9].shape[0]
        r = np.arange(nrows, dtype=np.float64)
        area = np.cos((-75.0 + 150.0 * (r + 0.5) / nrows) * (math.pi / 180.0)).astype(np.float32)
        return jax.shard_map(
            functools.partial(body, dims, area),
            mesh=mesh,
            in_specs=in_specs,
            out_specs=out_specs,
            check_vma=False,
        )(*args)

    return run
```

```python
import functools
import math

import jax
import jax.numpy as jnp
import numpy as np
from jax import lax
from jax.experimental import pallas as pl
from jax.experimental.pallas import tpu as pltpu
from jax.sharding import PartitionSpec as P

LANES = 128
SUB = 8
EDGE = 4
F32 = jnp.float32
BF16 = jnp.bfloat16
MESH = pl.DeviceIdType.MESH


def wrap(value, count):
    return jnp.where(value >= count, value - count, value)


def iota(shape, dim):
    return lax.broadcasted_iota(jnp.int32, shape, dim)


def turn(value, shift, axis):
    size = value.shape[axis]
    shift = shift % size
    return pltpu.roll(value, shift, axis) if shift else value


def position():
    return tuple(lax.axis_index(a) for a in ("role", "gy", "gx"))


def peer_of(dims, d):
    n_role, n_gy, n_gx = dims[:3]
    role, gy, gx = position()
    dx, dyr = d % n_gx, d // n_gx
    dy, dr = dyr % n_gy, dyr // n_gy
    return (wrap(role + dr, n_role), wrap(gy + dy, n_gy), wrap(gx + dx, n_gx))


def kernel(
    dims,
    temp_hbm,
    salt_hbm,
    zonal_hbm,
    merid_hbm,
    panel_hbm,
    kappa_hbm,
    land_hbm,
    start_hbm,
    cluster_hbm,
    area_hbm,
    band_hbm,
    out_ref,
    sums_ref,
    kappa_ref,
    land_ref,
    start_ref,
    cluster_ref,
    area_ref,
    band_ref,
    x0,
    x1,
    uv,
    means,
    halo_x,
    halo_uv,
    cols,
    band_rows,
    lat_send,
    lat,
    e_send,
    e_recv,
    placed,
    panel,
    shifted,
    result,
    gather,
    in_sems,
    small_sems,
    panel_sems,
    halo_send_sems,
    halo_recv_sems,
    a2a_send_sems,
    a2a_recv_sems,
    local_sems,
    e_send_sems,
    e_recv_sems,
    sum_sems,
):
    n_role, n_gy, n_gx, levels, cy, cx, trows, srows, nblk, sw, tb, groups = dims
    role, gy, gx = position()
    total = n_role * n_gy * n_gx
    me = (role * n_gy + gy) * n_gx + gx
    lev_grp = 16 // trows
    halves = levels // lev_grp
    lev_rows = lev_grp * trows
    half_rows = 3 * lev_rows
    nk = EDGE * levels
    peer = functools.partial(peer_of, dims)

    smalls = (
        (kappa_hbm, kappa_ref),
        (land_hbm, land_ref),
        (band_hbm, band_ref),
        (start_hbm, start_ref),
        (cluster_hbm, cluster_ref),
        (area_hbm, area_ref),
    )
    small_loads = [
        pltpu.make_async_copy(src, dst, small_sems.at[i]) for i, (src, dst) in enumerate(smalls)
    ]
    for load in small_loads:
        load.start()
    sources = ((temp_hbm, x0.at[0]), (salt_hbm, x0.at[1]), (zonal_hbm, uv.at[0]), (merid_hbm, uv.at[1]))
    loads = [pltpu.make_async_copy(src, dst, in_sems.at[i]) for i, (src, dst) in enumerate(sources)]
    for load in loads:
        load.start()
    panel_loads = [
        pltpu.make_async_copy(panel_hbm.at[j], panel.at[j], panel_sems.at[j]) for j in range(nblk)
    ]
    for load in panel_loads:
        load.start()

    barrier = pltpu.get_barrier_semaphore()
    greeted = set(range(1, n_gx)) | {d * n_gx for d in range(1, n_role * n_gy)}
    for dy in {1, n_gy - 1}:
        for dx in {1, n_gx - 1}:
            greeted.add(dy * n_gx + dx)
    greeted = sorted(greeted)
    for d in greeted:
        pl.semaphore_signal(barrier, inc=1, device_id=peer(d), device_id_type=MESH)

    has_below = gy > 0
    has_above = gy < n_gy - 1

    @pl.when(gy == 0)
    def _():
        halo_x[0] = jnp.zeros_like(halo_x[0])
        halo_uv[0] = jnp.zeros_like(halo_uv[0])
        for i in range(4):
            cols[i, pl.ds(0, SUB)] = jnp.zeros((SUB, LANES), F32)

    @pl.when(gy == n_gy - 1)
    def _():
        halo_x[1] = jnp.zeros_like(halo_x[1])
        halo_uv[1] = jnp.zeros_like(halo_uv[1])
        for i in range(4):
            cols[i, pl.ds(SUB + cy, SUB)] = jnp.zeros((SUB, LANES), F32)

    columns = n_gx * cx
    lat[columns // LANES] = jnp.zeros((halves * half_rows, LANES), BF16)

    def ocean_of(dy, dx):
        ty = gy + dy
        tx = wrap(gx + dx + n_gx, n_gx)
        number = jnp.full((1, cx), ty * n_gx + tx, jnp.int32)
        flag = jnp.where((jnp.full((1, cx), ty, jnp.int32) >= 0) & (jnp.full((1, cx), ty, jnp.int32) < n_gy), 1.0, 0.0)
        for i in range(land_ref.shape[0]):
            flag = jnp.where(jnp.full((1, cx), land_ref[i], jnp.int32) == number, 0.0, flag)
        return flag

    for load in small_loads:
        load.wait()
    ocean = ocean_of(0, 0)

    band_rows[...] = jnp.zeros_like(band_rows)
    for g in range(n_gx):
        band_rows[pl.ds(g * trows, trows), pl.ds(0, srows)] = band_ref[g].astype(F32)
    brows = band_rows.shape[0]
    out_r, in_r = n_gx * lev_rows, lev_grp * cy
    flat = band_rows[...].astype(BF16)
    ri, rq = iota((out_r, brows), 0), iota((out_r, brows), 1)
    pick_r = (lax.div(ri, lev_rows) == lax.div(rq, trows)) & (
        lax.rem(ri, trows) == lax.rem(rq, trows)
    )
    spread = jnp.dot(pick_r.astype(F32).astype(BF16), flat, preferred_element_type=F32)
    cs, cc = iota((LANES, in_r), 0), iota((LANES, in_r), 1)
    pick_c = (lax.rem(lax.rem(cc, cy), srows) == cs).astype(F32).astype(BF16)
    spread = jnp.dot(spread.astype(BF16), pick_c, preferred_element_type=F32)
    ai, ac = iota((out_r, in_r), 0), iota((out_r, in_r), 1)
    keep = (lax.div(lax.rem(ai, lev_rows), trows) == lax.div(ac, cy)) & (
        lax.div(lax.rem(ac, cy), srows) == lax.div(ai, lev_rows)
    )
    band = jnp.where(keep, spread, 0.0).astype(BF16)

    lane = iota((1, LANES), 1)
    quad = lax.div(lane, EDGE)
    col = lax.rem(lane, EDGE)

    for load in loads:
        load.wait()
    first = jnp.zeros((cy, LANES), F32)
    last = jnp.zeros((cy, LANES), F32)
    for q in range(4 * levels):
        kind, l = q // levels, q % levels
        source = x0.at[kind, l] if kind < 2 else uv.at[kind - 2, l]
        head = source[:, pl.ds(0, LANES)].astype(F32)
        tail = source[:, pl.ds(cx - LANES, LANES)].astype(F32)
        first = jnp.where(quad == q, turn(head, EDGE * q, 1), first)
        last = jnp.where(quad == q, turn(tail, EDGE * (q + 1), 1), last)
    cols[1, pl.ds(SUB, cy)] = first
    cols[2, pl.ds(SUB, cy)] = last

    west = wrap(gx + n_gx - 1, n_gx)
    east = wrap(gx + 1, n_gx)
    own_w, own_e = cols.at[1, pl.ds(SUB, cy)], cols.at[2, pl.ds(SUB, cy)]
    plan = [
        (None, None, own_w, cols.at[3, pl.ds(SUB, cy)], (role, gy, west)),
        (None, None, own_e, cols.at[0, pl.ds(SUB, cy)], (role, gy, east)),
    ]
    for side, (can_send, can_recv) in enumerate(((has_below, has_above), (has_above, has_below))):
        ty = gy - 1 if side == 0 else gy + 1
        mine = SUB if side == 0 else cy
        theirs = SUB + cy if side == 0 else 0
        for block, there, tx in ((1, 1, gx), (2, 2, gx), (1, 3, west), (2, 0, east)):
            plan.append(
                (
                    can_send,
                    can_recv,
                    cols.at[block, pl.ds(mine, SUB)],
                    cols.at[there, pl.ds(theirs, SUB)],
                    (role, ty, tx),
                )
            )
        row = 0 if side == 0 else cy - 2
        slot = 0 if side == 0 else SUB - 2
        for t, ref in enumerate((temp_hbm, salt_hbm)):
            plan.append(
                (
                    can_send,
                    can_recv,
                    ref.at[:, pl.ds(row, 2), :],
                    halo_x.at[1 - side, t, :, pl.ds(slot, 2), :],
                    (role, ty, gx),
                )
            )
        row = 0 if side == 0 else cy - SUB
        for t, ref in enumerate((zonal_hbm, merid_hbm)):
            plan.append(
                (
                    can_send,
                    can_recv,
                    ref.at[:, pl.ds(row, SUB), :],
                    halo_uv.at[1 - side, t],
                    (role, ty, gx),
                )
            )

    def when(cond, do):
        if cond is None:
            do()
        else:
            pl.when(cond)(do)

    halos = []
    for i, (can_send, can_recv, src, dst, target) in enumerate(plan):
        copy = pltpu.make_async_remote_copy(
            src_ref=src,
            dst_ref=dst,
            send_sem=halo_send_sems.at[i],
            recv_sem=halo_recv_sems.at[i],
            device_id=target,
            device_id_type=MESH,
        )
        halos.append((can_send, can_recv, copy))
    column_halos = halos[:2] + halos[2:6] + halos[10:14]
    row_halos = halos[6:10] + halos[14:18]

    pl.semaphore_wait(barrier, len(greeted))
    for can_send, _, copy in halos:
        when(can_send, copy.start)

    level0 = role * levels

    def advance(c, e, w, n, b, u, v, kap):
        return (1.0 - 4.0 * kap) * c + (kap * (e + w + n + b) - u * (e - w) - v * (n - b))

    def whole(c, u, v, kap):
        return advance(
            c, turn(c, -1, 1), turn(c, 1, 1), turn(c, -1, 0), turn(c, 1, 0), u, v, kap
        )

    def density(temp, salt, factor):
        return 0.78 * salt - factor * temp - 0.02 * temp * temp

    def factor_of(l):
        return 0.17 * (1.0 + 0.03 * (level0 + l).astype(F32))

    wide = iota((1, cx), 1)
    at_edge = (wide < 2) | (wide >= cx - 2)
    tiles = cx // LANES
    order = sorted(range(1, n_gx), key=lambda d: -min(d, n_gx - d))
    at_end = (gx == 0) | (gx == n_gx - 1)

    def bulk(h, d):
        target = wrap(gx + d, n_gx)
        return target, pltpu.make_async_remote_copy(
            src_ref=lat_send.at[h, target],
            dst_ref=lat.at[pl.ds(gx * tiles, tiles), pl.ds(h * half_rows, half_rows)],
            send_sem=a2a_send_sems.at[h, d],
            recv_sem=a2a_recv_sems.at[h, d],
            device_id=(role, gy, target),
            device_id_type=MESH,
        )

    def local(h):
        return pltpu.make_async_copy(
            lat_send.at[h, gx],
            lat.at[pl.ds(gx * tiles, tiles), pl.ds(h * half_rows, half_rows)],
            local_sems.at[h],
        )

    def stage(h, g, f, rows):
        for i in range(tiles):
            lat_send[h, g, i, pl.ds(f * lev_rows, lev_rows)] = rows[
                :, i * LANES : (i + 1) * LANES
            ]

    for h in range(halves):
        for l in range(h * lev_grp, (h + 1) * lev_grp):
            u = uv[0, l].astype(F32) * (0.5 * ocean)
            v = uv[1, l].astype(F32) * (0.5 * ocean)
            kap = kappa_ref[l] * ocean
            one = [whole(x0[t, l], u, v, kap) for t in range(2)]
            two = [whole(one[t], u, v, kap) for t in range(2)]
            factor = factor_of(l)
            r1 = density(one[0], one[1], factor)
            r2 = density(two[0], two[1], factor)
            x1[0, l] = one[0]
            x1[1, l] = one[1]
            means[0, l] = (0.5 * (one[0] + two[0])).astype(BF16)
            means[1, l] = (0.5 * (one[1] + two[1])).astype(BF16)
            means[2, l] = (0.5 * (r1 + r2)).astype(BF16)
        for f in range(3):
            rows = means[f, pl.ds(h * lev_grp, lev_grp)].reshape(in_r, cx)
            got = jnp.dot(
                band[lev_rows : out_r - lev_rows], rows, preferred_element_type=F32
            )
            got = jnp.where(at_edge, 0.0, got).astype(BF16)
            for g in range(1, n_gx - 1):
                stage(h, g, f, got[(g - 1) * lev_rows : g * lev_rows])
        for d in order:
            target, copy = bulk(h, d)
            pl.when((target > 0) & (target < n_gx - 1))(copy.start)
        pl.when(jnp.logical_not(at_end))(local(h).start)

    for _, can_recv, copy in column_halos:
        when(can_recv, copy.wait_recv)
    cye = cy + 2 * SUB
    row_e = iota((cye, 1), 0)
    kap_l = jnp.zeros((1, LANES), F32)
    factor_l = jnp.zeros((1, LANES), F32)
    lane_level = lax.div(lax.rem(lane, nk), EDGE)
    for l in range(levels):
        kap_l = jnp.where(lane_level == l, kappa_ref[l], kap_l)
        factor_l = jnp.where(lane_level == l, factor_of(l), factor_l)

    flags = {(dy, dx): ocean_of(dy, dx)[:, :LANES] for dy in (-1, 0, 1) for dx in (-1, 0, 1)}

    def coefficients(i, dx):
        block = cols[i]
        oc = jnp.where(
            row_e < SUB, flags[-1, dx], jnp.where(row_e < SUB + cy, flags[0, dx], flags[1, dx])
        )
        half = 0.5 * oc
        u = jnp.where(lane < nk, turn(block, -2 * nk, 1), turn(block, -nk, 1)) * half
        v = jnp.where(lane < nk, turn(block, -3 * nk, 1), turn(block, -2 * nk, 1)) * half
        return u, v, kap_l * oc

    def step_left(left, right, coef):
        e = jnp.where(col == EDGE - 1, turn(right, EDGE - 1, 1), turn(left, -1, 1))
        return advance(left, e, turn(left, 1, 1), turn(left, -1, 0), turn(left, 1, 0), *coef)

    def step_right(left, right, coef):
        w = jnp.where(col == 0, turn(left, 1 - EDGE, 1), turn(right, 1, 1))
        return advance(
            right, turn(right, -1, 1), w, turn(right, -1, 0), turn(right, 1, 0), *coef
        )

    own = coefficients(1, 0)
    left1 = step_left(cols[0], cols[1], coefficients(0, -1))
    west1 = step_right(cols[0], cols[1], own)
    west2 = step_right(left1, west1, own)
    own = coefficients(2, 0)
    east1 = step_left(cols[2], cols[3], own)
    right1 = step_right(cols[2], cols[3], coefficients(3, 1))
    east2 = step_left(east1, right1, own)
    both1 = jnp.where(col < 2, west1, east1)[SUB : SUB + cy]
    both2 = jnp.where(col < 2, west2, east2)[SUB : SUB + cy]
    rho = 0.5 * (
        density(both1, turn(both1, -nk, 1), factor_l)
        + density(both2, turn(both2, -nk, 1), factor_l)
    )
    packed = jnp.where(
        lane < 2 * nk,
        0.5 * (both1 + both2),
        jnp.where(lane < 3 * nk, turn(rho, 2 * nk, 1), 0.0),
    ).astype(BF16)
    narrow = n_gx * trows
    thin = jnp.dot(flat[:narrow], pick_c[:, :cy], preferred_element_type=F32)
    ei, ec = iota((narrow, cy), 0), iota((narrow, cy), 1)
    thin = jnp.where(lax.div(ec, srows) == lax.div(ei, trows), thin, 0.0).astype(BF16)
    edge_lat = jnp.dot(thin, packed, preferred_element_type=F32).astype(BF16)
    for g in range(n_gx):
        e_send[g] = edge_lat[g * trows : (g + 1) * trows]

    e_copies = []
    for d in order:
        target = wrap(gx + d, n_gx)
        copy = pltpu.make_async_remote_copy(
            src_ref=e_send.at[target],
            dst_ref=e_recv.at[gx],
            send_sem=e_send_sems.at[d],
            recv_sem=e_recv_sems.at[d],
            device_id=(role, gy, target),
            device_id_type=MESH,
        )
        copy.start()
        e_copies.append(copy)
    e_recv[pl.ds(gx, 1)] = e_send[pl.ds(gx, 1)]

    for _, can_recv, copy in row_halos:
        when(can_recv, copy.wait_recv)
    sub8 = iota((SUB, 1), 0)
    ocean_below, ocean_above = ocean_of(-1, 0), ocean_of(1, 0)

    def up(a, b):
        return jnp.where(sub8 == SUB - 1, turn(b, -1, 0), turn(a, -1, 0))

    def down(a, b):
        return jnp.where(sub8 == 0, turn(a, 1, 0), turn(b, 1, 0))

    def rows_step(c, n, b, u, v, kap):
        return advance(c, turn(c, -1, 1), turn(c, 1, 1), n, b, u, v, kap)

    for l in range(levels):
        kap = kappa_ref[l] * ocean
        factor = factor_of(l)
        flow = [uv[i, l, pl.ds(0, 16)].astype(F32)[:SUB] * (0.5 * ocean) for i in range(2)]
        other = [halo_uv[0, i, l].astype(F32) * (0.5 * ocean_below) for i in range(2)]
        kap_o = kappa_ref[l] * ocean_below
        ones, twos = [], []
        for t in range(2):
            far, edge, near = halo_x[0, t, l], x0[t, l, pl.ds(0, SUB)], x0[t, l, pl.ds(SUB, SUB)]
            out1 = rows_step(far, up(far, edge), turn(far, 1, 0), *other, kap_o)
            in1 = rows_step(edge, up(edge, near), down(far, edge), *flow, kap)
            ones.append(in1)
            next1 = x1[t, l, pl.ds(SUB, SUB)]
            twos.append(rows_step(in1, up(in1, next1), down(out1, in1), *flow, kap))
        r = density(*ones, factor) + density(*twos, factor)
        for f, value in enumerate((ones[0] + twos[0], ones[1] + twos[1], r)):
            means[f, l, pl.ds(0, SUB)] = (0.5 * value).astype(BF16)

        flow = [uv[i, l, pl.ds(cy - 16, 16)].astype(F32)[SUB:] * (0.5 * ocean) for i in range(2)]
        other = [halo_uv[1, i, l].astype(F32) * (0.5 * ocean_above) for i in range(2)]
        kap_o = kappa_ref[l] * ocean_above
        ones, twos = [], []
        for t in range(2):
            far = halo_x[1, t, l]
            edge = x0[t, l, pl.ds(cy - SUB, SUB)]
            near = x0[t, l, pl.ds(cy - 2 * SUB, SUB)]
            out1 = rows_step(far, turn(far, -1, 0), down(edge, far), *other, kap_o)
            in1 = rows_step(edge, up(edge, far), down(near, edge), *flow, kap)
            ones.append(in1)
            next1 = x1[t, l, pl.ds(cy - 2 * SUB, SUB)]
            twos.append(rows_step(in1, up(in1, out1), down(next1, in1), *flow, kap))
        r = density(*ones, factor) + density(*twos, factor)
        for f, value in enumerate((ones[0] + twos[0], ones[1] + twos[1], r)):
            means[f, l, pl.ds(cy - SUB, SUB)] = (0.5 * value).astype(BF16)

    ends = jnp.concatenate([band[:lev_rows], band[out_r - lev_rows :]], axis=0)
    for h in range(halves):
        for f in range(3):
            rows = means[f, pl.ds(h * lev_grp, lev_grp)].reshape(in_r, cx)
            got = jnp.dot(ends, rows, preferred_element_type=F32)
            got = jnp.where(at_edge, 0.0, got).astype(BF16)
            stage(h, 0, f, got[:lev_rows])
            stage(h, n_gx - 1, f, got[lev_rows:])
        for d in order:
            target, copy = bulk(h, d)
            pl.when((target == 0) | (target == n_gx - 1))(copy.start)
        pl.when(at_end)(local(h).start)

    depth = sw + LANES
    sub = iota((1, SUB, 1), 1)

    def tile_of(j):
        return lax.div(start_ref[j], LANES)

    blank = jnp.zeros((SUB, tb), F32)
    for j in range(nblk):
        panel_loads[j].wait()
        off = jnp.full((1, tb), start_ref[j] - tile_of(j) * LANES, jnp.int32)
        rows = panel[j].astype(F32)
        parts = [rows[i * SUB : (i + 1) * SUB] for i in range(sw // SUB)]
        bit = 1
        while bit < SUB:
            taken = lax.rem(lax.div(off, bit), 2) == 1
            low = sub8 < bit
            ring = [turn(part, bit, 0) for part in parts] + [blank]
            parts = [
                jnp.where(
                    taken,
                    jnp.where(low, ring[i - 1] if i else blank, ring[i]),
                    parts[i] if i < len(parts) else blank,
                )
                for i in range(len(ring))
            ] if bit == 1 else [
                jnp.where(taken, jnp.where(low, ring[i - 1] if i else blank, ring[i]), parts[i])
                for i in range(len(parts))
            ]
            bit *= 2
        step = 1
        while step * SUB < LANES:
            taken = lax.rem(lax.div(off, step * SUB), 2) == 1
            longer = len(parts) + step
            parts = [
                jnp.where(
                    taken,
                    parts[i - step] if i >= step else blank,
                    parts[i] if i < len(parts) else blank,
                )
                for i in range(longer)
            ]
            step *= 2
        assert len(parts) == depth // SUB
        shifted[j] = jnp.concatenate(parts, axis=0).astype(BF16)

    glanes = gather.shape[2]
    lanes = iota((1, glanes), 1)
    labels = lax.rem(lanes, groups)

    def add_area(r, so_far):
        return so_far + jnp.where(labels == cluster_ref[r], area_ref[r], 0.0)

    area_sum = lax.fori_loop(
        0, cluster_ref.shape[0], add_area, jnp.zeros((1, glanes), F32), unroll=8
    )
    thick_total = sum(1.0 + 0.25 * k for k in range(levels * n_role))
    denom = area_sum * (thick_total * nblk * tb)
    first_row = (gy * n_gx + gx) * trows
    out_rows = halves * half_rows
    orow = iota((out_rows, 1), 0)
    ti = lax.rem(orow, trows)
    hot = jnp.zeros((out_rows, glanes), F32)
    for t in range(trows):
        row_hot = jnp.where(labels == cluster_ref[first_row + t], area_ref[first_row + t], 0.0)
        hot = jnp.where(ti == t, row_hot, hot)
    olevel = lax.div(orow, half_rows) * lev_grp + lax.div(lax.rem(orow, lev_rows), trows)
    ofield = lax.div(lax.rem(orow, half_rows), lev_rows)
    thick = 1.0 + 0.25 * (level0 + olevel).astype(F32)
    field = lax.div(lanes, groups)
    hot = jnp.where(ofield == field, hot * thick, 0.0)

    pk, pc = iota((LANES, cx), 0), iota((LANES, cx), 1)
    place = jnp.where(pc < 2, pc, jnp.where(pc >= cx - 2, pc - (cx - EDGE), -1))
    place = (place == lax.rem(pk, EDGE)).astype(F32).astype(BF16)
    mine_q = ofield * levels + olevel
    for copy in e_copies:
        copy.wait_recv()
    for s in range(n_gx):
        block = e_recv[s].astype(F32)
        tall = jnp.concatenate([block] * (out_rows // trows), axis=0)
        tall = jnp.where(quad == mine_q, tall, 0.0).astype(BF16)
        put = jnp.dot(tall, place, preferred_element_type=F32).astype(BF16)
        for i in range(tiles):
            placed[s * tiles + i] = put[:, i * LANES : (i + 1) * LANES]

    for h in range(halves):
        for d in order:
            bulk(h, d)[1].wait_recv()
        local(h).wait()
    for i in range(n_gx * tiles):
        lat[i] = lat[i] + placed[i]
    squares = jnp.zeros((out_rows, tb), F32)
    for j in range(nblk):
        tile = tile_of(j)
        window = jnp.concatenate([lat[tile + i] for i in range(depth // LANES)], axis=1)
        values = jnp.dot(window, shifted[j], preferred_element_type=F32)
        squares = squares + values * values
        result[:, pl.ds(j * tb, tb)] = values
    weighted = jnp.sum(squares, axis=1, keepdims=True) * hot
    part = jnp.sum(weighted, axis=0, keepdims=True) / denom

    def for_others(do):
        if total <= 64:
            for d in range(1, total):
                do(peer(d))
        else:

            @pl.loop(1, total)
            def _(d):
                do(peer(d))

    def send(device):
        pltpu.make_async_remote_copy(
            src_ref=gather.at[me],
            dst_ref=gather.at[me],
            send_sem=sum_sems.at[0],
            recv_sem=sum_sems.at[1],
            device_id=device,
            device_id_type=MESH,
        ).start()

    gather[me] = part
    for_others(send)

    for h in range(halves):
        for f in range(3):
            for i in range(lev_grp):
                row = h * half_rows + f * lev_rows + i * trows
                out_ref[f, h * lev_grp + i] = result[pl.ds(row, trows), :].astype(BF16)

    for can_send, _, copy in halos:
        when(can_send, copy.wait_send)
    for h in range(halves):
        for d in order:
            bulk(h, d)[1].wait_send()
    for copy in e_copies:
        copy.wait_send()
    every = gather.at[pl.ds(0, total - 1)]
    for i in (1, 0):
        pltpu.make_async_copy(every, every, sum_sems.at[i]).wait()
    sums = jnp.sum(gather[...], axis=0)
    for f in range(3):
        sums_ref[pl.ds(f, 1), :] = turn(sums, -f * groups, 1)[:, :groups]


def store_kernel(remapped_ref, sums_ref, remapped_hbm, sums_hbm, sems):
    copies = [
        pltpu.make_async_copy(remapped_ref, remapped_hbm, sems.at[0]),
        pltpu.make_async_copy(sums_ref, sums_hbm, sems.at[1]),
    ]
    for copy in copies:
        copy.start()
    for copy in copies:
        copy.wait()


def body(
    dims,
    area,
    thermal_anomaly,
    saltiness_anomaly,
    zonal_flow_fraction,
    meridional_flow_fraction,
    mixing_coefficient,
    continent_patch_numbering,
    parallel_band_coefficients,
    meridian_panel_coefficients,
    panel_starting_source_meridian,
    target_parallel_cluster,
):
    n_role, n_gy, n_gx, levels, cy, cx, trows, srows, nblk, sw, tb, groups = dims
    total = n_role * n_gy * n_gx
    lev_grp = 16 // trows
    halves = levels // lev_grp
    half_rows = 3 * lev_grp * trows
    glanes = -(-3 * groups // LANES) * LANES
    hbm = pl.BlockSpec(memory_space=pltpu.MemorySpace.HBM)
    vmem = pl.BlockSpec(memory_space=pltpu.VMEM)
    brows = -(-n_gx * trows // LANES) * LANES
    dma = pltpu.SemaphoreType.DMA
    columns = n_gx * cx
    out_rows = halves * half_rows
    remapped, sums = pl.pallas_call(
        functools.partial(kernel, dims),
        out_shape=(
            jax.ShapeDtypeStruct((3, levels, trows, nblk * tb), BF16),
            jax.ShapeDtypeStruct((3, groups), F32),
        ),
        in_specs=[hbm] * 11,
        out_specs=(vmem, vmem),
        scratch_shapes=[
            pltpu.SMEM(mixing_coefficient.shape, F32),
            pltpu.SMEM(continent_patch_numbering.shape, jnp.int32),
            pltpu.SMEM(panel_starting_source_meridian.shape, jnp.int32),
            pltpu.SMEM(target_parallel_cluster.shape, jnp.int32),
            pltpu.SMEM(area.shape, F32),
            pltpu.VMEM(parallel_band_coefficients.shape, BF16),
            pltpu.VMEM((2, levels, cy, cx), F32),
            pltpu.VMEM((2, levels, cy, cx), F32),
            pltpu.VMEM((2, levels, cy, cx), BF16),
            pltpu.VMEM((3, levels, cy, cx), BF16),
            pltpu.VMEM((2, 2, levels, SUB, cx), F32),
            pltpu.VMEM((2, 2, levels, SUB, cx), BF16),
            pltpu.VMEM((4, cy + 2 * SUB, LANES), F32),
            pltpu.VMEM((brows, LANES), F32),
            pltpu.VMEM((halves, n_gx, cx // LANES, half_rows, LANES), BF16),
            pltpu.VMEM((columns // LANES + 1, out_rows, LANES), BF16),
            pltpu.VMEM((n_gx, trows, LANES), BF16),
            pltpu.VMEM((n_gx, trows, LANES), BF16),
            pltpu.VMEM((columns // LANES, out_rows, LANES), BF16),
            pltpu.VMEM((nblk, sw, tb), BF16),
            pltpu.VMEM((nblk, sw + LANES, tb), BF16),
            pltpu.VMEM((out_rows, nblk * tb), F32),
            pltpu.VMEM((total, 1, glanes), F32),
            dma((4,)),
            dma((6,)),
            dma((nblk,)),
            dma((18,)),
            dma((18,)),
            dma((halves, n_gx)),
            dma((halves, n_gx)),
            dma((halves,)),
            dma((n_gx,)),
            dma((n_gx,)),
            dma((2,)),
        ],
        compiler_params=pltpu.CompilerParams(
            collective_id=0, has_side_effects=True, vmem_limit_bytes=26 * 1024 * 1024
        ),
        name="ocean",
    )(
        *(
            pltpu.with_memory_space_constraint(array, pltpu.MemorySpace.HBM)
            for array in (
                thermal_anomaly,
                saltiness_anomaly,
                zonal_flow_fraction,
                meridional_flow_fraction,
                meridian_panel_coefficients,
                mixing_coefficient,
                continent_patch_numbering,
                panel_starting_source_meridian,
                target_parallel_cluster,
                jnp.asarray(area),
                parallel_band_coefficients,
            )
        )
    )
    return pl.pallas_call(
        store_kernel,
        out_shape=(
            jax.ShapeDtypeStruct(remapped.shape, BF16),
            jax.ShapeDtypeStruct(sums.shape, F32),
        ),
        in_specs=[vmem, vmem],
        out_specs=(hbm, hbm),
        scratch_shapes=[dma((2,))],
        compiler_params=pltpu.CompilerParams(vmem_limit_bytes=4 * 1024 * 1024),
        name="store",
    )(remapped, sums)


def solution(mesh):
    in_specs = (
        P("role", "gy", "gx"),
        P("role", "gy", "gx"),
        P("role", "gy", "gx"),
        P("role", "gy", "gx"),
        P("role"),
        P(),
        P("gy", None, None),
        P(),
        P(),
        P(),
    )
    out_specs = (P(None, "role", ("gy", "gx"), None), P())

    def run(*args):
        n_role, n_gy, n_gx = (mesh.shape[a] for a in ("role", "gy", "gx"))
        levels, rows, cols = args[0].shape
        _, trows, srows = args[6].shape
        nblk, sw, tb = args[7].shape
        dims = (
            n_role,
            n_gy,
            n_gx,
            levels // n_role,
            rows // n_gy,
            cols // n_gx,
            trows,
            srows,
            nblk,
            sw,
            tb,
            4 * n_gy,
        )
        nrows = args[9].shape[0]
        r = np.arange(nrows, dtype=np.float64)
        area = np.cos((-75.0 + 150.0 * (r + 0.5) / nrows) * (math.pi / 180.0)).astype(np.float32)
        return jax.shard_map(
            functools.partial(body, dims, area),
            mesh=mesh,
            in_specs=in_specs,
            out_specs=out_specs,
            check_vma=False,
        )(*args)

    return run
```

```python
import functools
import math

import jax
import jax.numpy as jnp
import numpy as np
from jax import lax
from jax.experimental import pallas as pl
from jax.experimental.pallas import tpu as pltpu
from jax.sharding import PartitionSpec as P

LANES = 128
SUB = 8
EDGE = 4
SPLIT = 3
F32 = jnp.float32
BF16 = jnp.bfloat16
MESH = pl.DeviceIdType.MESH


def wrap(value, count):
    return jnp.where(value >= count, value - count, value)


def iota(shape, dim):
    return lax.broadcasted_iota(jnp.int32, shape, dim)


def turn(value, shift, axis):
    size = value.shape[axis]
    shift = shift % size
    return pltpu.roll(value, shift, axis) if shift else value


def partner(index, d, count):
    if count & (count - 1):
        return wrap(index + d, count)
    other = index
    for bit in range(count.bit_length() - 1):
        if d >> bit & 1:
            step = 1 << bit
            other = other + step - 2 * step * lax.rem(lax.div(index, step), 2)
    return other


def position():
    return tuple(lax.axis_index(a) for a in ("role", "gy", "gx"))


def peer_of(dims, d):
    n_role, n_gy, n_gx = dims[:3]
    role, gy, gx = position()
    dx, dyr = d % n_gx, d // n_gx
    dy, dr = dyr % n_gy, dyr // n_gy
    return (wrap(role + dr, n_role), wrap(gy + dy, n_gy), wrap(gx + dx, n_gx))


def kernel(
    dims,
    temp_hbm,
    salt_hbm,
    zonal_hbm,
    merid_hbm,
    panel_hbm,
    kappa_hbm,
    land_hbm,
    start_hbm,
    cluster_hbm,
    area_hbm,
    band_hbm,
    out_ref,
    sums_ref,
    kappa_ref,
    land_ref,
    start_ref,
    cluster_ref,
    area_ref,
    band_ref,
    x0,
    x1,
    uv,
    means,
    halo_x,
    halo_uv,
    cols,
    fold_send,
    fold_recv,
    chosen,
    band_rows,
    lat_send,
    lat,
    e_send,
    e_recv,
    placed,
    panel,
    shifted,
    result,
    gather,
    in_sems,
    small_sems,
    panel_sems,
    halo_send_sems,
    halo_recv_sems,
    a2a_send_sems,
    a2a_recv_sems,
    local_sems,
    e_send_sems,
    e_recv_sems,
    sum_sems,
):
    n_role, n_gy, n_gx, levels, cy, cx, trows, srows, nblk, sw, tb, groups = dims
    role, gy, gx = position()
    total = n_role * n_gy * n_gx
    me = (role * n_gy + gy) * n_gx + gx
    lev_grp = 16 // trows
    halves = levels // lev_grp
    lev_rows = lev_grp * trows
    half_rows = 3 * lev_rows
    nk = EDGE * levels
    peer = functools.partial(peer_of, dims)

    smalls = (
        (kappa_hbm, kappa_ref),
        (land_hbm, land_ref),
        (band_hbm, band_ref),
        (start_hbm, start_ref),
        (cluster_hbm, cluster_ref),
        (area_hbm, area_ref),
    )
    small_loads = [
        pltpu.make_async_copy(src, dst, small_sems.at[i]) for i, (src, dst) in enumerate(smalls)
    ]
    for load in small_loads:
        load.start()
    sources = ((temp_hbm, x0.at[0]), (salt_hbm, x0.at[1]), (zonal_hbm, uv.at[0]), (merid_hbm, uv.at[1]))
    loads = []
    for h in range(halves):
        part = pl.ds(h * lev_grp, lev_grp)
        loads.append(
            [
                pltpu.make_async_copy(src.at[part], dst.at[part], in_sems.at[h, i])
                for i, (src, dst) in enumerate(sources)
            ]
        )
        for load in loads[h]:
            load.start()
    panel_loads = [
        pltpu.make_async_copy(panel_hbm.at[j], panel.at[j], panel_sems.at[j]) for j in range(nblk)
    ]

    barrier = pltpu.get_barrier_semaphore()
    greeted = set(range(1, n_gx)) | {d * n_gx for d in range(1, n_role * n_gy)}
    for dy in {1, n_gy - 1}:
        for dx in {1, n_gx - 1}:
            greeted.add(dy * n_gx + dx)
    greeted = sorted(greeted)
    for d in greeted:
        pl.semaphore_signal(barrier, inc=1, device_id=peer(d), device_id_type=MESH)

    lane = iota((1, LANES), 1)
    quad = lax.div(lane, EDGE)
    col = lax.rem(lane, EDGE)
    has_below = gy > 0
    has_above = gy < n_gy - 1

    @pl.when(gy == 0)
    def _():
        halo_x[0] = jnp.zeros_like(halo_x[0])
        halo_uv[0] = jnp.zeros_like(halo_uv[0])
        for i in range(4):
            cols[i, pl.ds(0, SUB)] = jnp.zeros((SUB, LANES), F32)

    @pl.when(gy == n_gy - 1)
    def _():
        halo_x[1] = jnp.zeros_like(halo_x[1])
        halo_uv[1] = jnp.zeros_like(halo_uv[1])
        for i in range(4):
            cols[i, pl.ds(SUB + cy, SUB)] = jnp.zeros((SUB, LANES), F32)

    columns = n_gx * cx
    for h in range(halves):
        lat[h][columns // LANES] = jnp.zeros((half_rows, LANES), BF16)

    def ocean_of(dy, dx):
        ty = gy + dy
        tx = wrap(gx + dx + n_gx, n_gx)
        number = jnp.full((1, cx), ty * n_gx + tx, jnp.int32)
        flag = jnp.where((jnp.full((1, cx), ty, jnp.int32) >= 0) & (jnp.full((1, cx), ty, jnp.int32) < n_gy), 1.0, 0.0)
        for i in range(land_ref.shape[0]):
            flag = jnp.where(jnp.full((1, cx), land_ref[i], jnp.int32) == number, 0.0, flag)
        return flag

    for load in small_loads:
        load.wait()
    ocean = ocean_of(0, 0)

    chosen[...] = jnp.zeros_like(chosen)
    for q in range(2 * levels):
        for side, (base, top) in enumerate(((0, 0), (LANES - 16, LANES - EDGE))):
            ck, cl = iota((16, LANES), 0) + base, iota((16, LANES), 1)
            hit = (ck >= top) & (ck < top + EDGE) & (ck - top == cl - 2 * nk - EDGE * q)
            chosen[side, pl.ds(q * LANES + base, 16)] = jnp.where(hit, 1.0, 0.0).astype(BF16)
    band_rows[...] = jnp.zeros_like(band_rows)
    for g in range(n_gx):
        band_rows[pl.ds(g * trows, trows), pl.ds(0, srows)] = band_ref[g].astype(F32)
    brows = band_rows.shape[0]
    out_r, in_r = n_gx * lev_rows, lev_grp * cy
    flat = band_rows[...].astype(BF16)
    ri, rq = iota((out_r, brows), 0), iota((out_r, brows), 1)
    pick_r = (lax.div(ri, lev_rows) == lax.div(rq, trows)) & (
        lax.rem(ri, trows) == lax.rem(rq, trows)
    )
    spread = jnp.dot(pick_r.astype(F32).astype(BF16), flat, preferred_element_type=F32)
    cs, cc = iota((LANES, in_r), 0), iota((LANES, in_r), 1)
    pick_c = (lax.rem(lax.rem(cc, cy), srows) == cs).astype(F32).astype(BF16)
    spread = jnp.dot(spread.astype(BF16), pick_c, preferred_element_type=F32)
    ai, ac = iota((out_r, in_r), 0), iota((out_r, in_r), 1)
    keep = (lax.div(lax.rem(ai, lev_rows), trows) == lax.div(ac, cy)) & (
        lax.div(lax.rem(ac, cy), srows) == lax.div(ai, lev_rows)
    )
    band = jnp.where(keep, spread, 0.0).astype(BF16)

    level0 = role * levels

    def stencil(u, v, kap):
        return 1.0 - 4.0 * kap, kap - u, kap + u, kap - v, kap + v

    def advance(c, e, w, n, b, coef):
        own, to_e, to_w, to_n, to_b = coef
        return (own * c + (to_e * e + to_w * w)) + (to_n * n + to_b * b)

    def whole(c, coef):
        tiles_of = range(len(c))
        left = [turn(a, -1, 1) for a in c]
        right = [turn(a, 1, 1) for a in c]
        out = []
        for i in tiles_of:
            e = jnp.where(lane == LANES - 1, left[i + 1], left[i]) if i + 1 < len(c) else left[i]
            w = jnp.where(lane == 0, right[i - 1], right[i]) if i else right[i]
            out.append(advance(c[i], e, w, turn(c[i], -1, 0), turn(c[i], 1, 0), coef[i]))
        return out

    def mean_fields(t1, s1, t2, s2, factor):
        t, s = t1 + t2, s1 + s2
        rho = 0.39 * s - (0.5 * factor) * t - 0.01 * (t1 * t1 + t2 * t2)
        return 0.5 * t, 0.5 * s, rho

    def factor_of(l):
        return 0.17 * (1.0 + 0.03 * (level0 + l).astype(F32))

    flag0 = ocean[:, :LANES]
    half0 = 0.5 * flag0
    wide = iota((1, cx), 1)
    at_edge = (wide < 2) | (wide >= cx - 2)
    tiles = cx // LANES
    order = list(range(n_gx - 1, 0, -1))
    at_end = (gx == 0) | (gx == n_gx - 1)

    def bulk(h, d):
        target = partner(gx, d, n_gx)
        return target, pltpu.make_async_remote_copy(
            src_ref=lat_send.at[h, target],
            dst_ref=lat[h].at[pl.ds(gx * tiles, tiles)],
            send_sem=a2a_send_sems.at[h, d],
            recv_sem=a2a_recv_sems.at[h, d],
            device_id=(role, gy, target),
            device_id_type=MESH,
        )

    def local(h):
        return pltpu.make_async_copy(
            lat_send.at[h, gx],
            lat[h].at[pl.ds(gx * tiles, tiles)],
            local_sems.at[h],
        )

    def stage(h, g, f, rows):
        for i in range(tiles):
            lat_send[h, g, i, pl.ds(f * lev_rows, lev_rows)] = rows[
                :, i * LANES : (i + 1) * LANES
            ]

    def main_levels(first_level, last_level):
        for l in range(first_level, last_level):
            kap = kappa_ref[l] * flag0
            spans = [pl.ds(i * LANES, LANES) for i in range(tiles)]
            coef = [
                stencil(
                    uv[0, l, :, span].astype(F32) * half0, uv[1, l, :, span].astype(F32) * half0, kap
                )
                for span in spans
            ]
            one = [whole([x0[t, l, :, span] for span in spans], coef) for t in range(2)]
            two = [whole(one[t], coef) for t in range(2)]
            factor = factor_of(l)
            for i, span in enumerate(spans):
                x1[0, l, :, span] = one[0][i]
                x1[1, l, :, span] = one[1][i]
                fields = mean_fields(one[0][i], one[1][i], two[0][i], two[1][i], factor)
                for f in range(3):
                    means[f, l, :, span] = fields[f].astype(BF16)

    def main_lat(h):
        for f in range(3):
            rows = means[f, pl.ds(h * lev_grp, lev_grp)].reshape(in_r, cx)
            got = jnp.dot(band[lev_rows : out_r - lev_rows], rows, preferred_element_type=F32)
            got = jnp.where(at_edge, 0.0, got).astype(BF16)
            for g in range(1, n_gx - 1):
                stage(h, g, f, got[(g - 1) * lev_rows : g * lev_rows])

    def held(target):
        return (target == n_gx // 2 - 1) | (target == n_gx // 2)

    def send_half(h):
        for d in order:
            target, copy = bulk(h, d)
            now = (target > 0) & (target < n_gx - 1)
            if h == halves - 1:
                now = now & jnp.logical_not(held(target))
            pl.when(now)(copy.start)
        pl.when(jnp.logical_not(at_end))(local(h).start)

    for load in loads[0]:
        load.wait()
    main_levels(0, SPLIT)
    for later in loads[1:]:
        for load in later:
            load.wait()
    packed = []
    for side, edge in enumerate((pl.ds(0, LANES), pl.ds(cx - LANES, LANES))):
        block = jnp.concatenate(
            [uv[q // levels, q % levels, :, edge] for q in range(2 * levels)], axis=1
        )
        block = jnp.dot(block, chosen[side], preferred_element_type=F32)
        for q in range(2 * levels):
            tile = x0[q // levels, q % levels, :, edge]
            block = jnp.where(quad == q, turn(tile, EDGE * (q + side), 1), block)
        packed.append(block)
    first, last = packed
    cols[1, pl.ds(SUB, cy)] = first
    cols[2, pl.ds(SUB, cy)] = last
    mid = cy // 2

    def fold(block):
        return jnp.where(lane < 2 * nk, block[:mid], turn(block[mid:], 2 * nk, 1))

    fold_send[0] = fold(jnp.where(col < 2, first, turn(first, 2 - 2 * nk, 1)))
    fold_send[1] = fold(jnp.where(col < 2, turn(last, -2 - 2 * nk, 1), last))

    west = wrap(gx + n_gx - 1, n_gx)
    east = wrap(gx + 1, n_gx)
    plan = [
        (None, None, fold_send.at[0], fold_recv.at[0], (role, gy, west)),
        (None, None, fold_send.at[1], fold_recv.at[1], (role, gy, east)),
    ]
    for side, (can_send, can_recv) in enumerate(((has_below, has_above), (has_above, has_below))):
        ty = gy - 1 if side == 0 else gy + 1
        mine = SUB if side == 0 else cy
        theirs = SUB + cy if side == 0 else 0
        for block, there, tx in ((1, 1, gx), (2, 2, gx), (1, 3, west), (2, 0, east)):
            plan.append(
                (
                    can_send,
                    can_recv,
                    cols.at[block, pl.ds(mine, SUB)],
                    cols.at[there, pl.ds(theirs, SUB)],
                    (role, ty, tx),
                )
            )
        row = 0 if side == 0 else cy - 2
        slot = 0 if side == 0 else SUB - 2
        for t, ref in enumerate((temp_hbm, salt_hbm)):
            plan.append(
                (
                    can_send,
                    can_recv,
                    ref.at[:, pl.ds(row, 2), :],
                    halo_x.at[1 - side, t, :, pl.ds(slot, 2), :],
                    (role, ty, gx),
                )
            )
        row = 0 if side == 0 else cy - SUB
        for t, ref in enumerate((zonal_hbm, merid_hbm)):
            plan.append(
                (
                    can_send,
                    can_recv,
                    ref.at[:, pl.ds(row, SUB), :],
                    halo_uv.at[1 - side, t],
                    (role, ty, gx),
                )
            )

    def when(cond, do):
        if cond is None:
            do()
        else:
            pl.when(cond)(do)

    halos = []
    for i, (can_send, can_recv, src, dst, target) in enumerate(plan):
        copy = pltpu.make_async_remote_copy(
            src_ref=src,
            dst_ref=dst,
            send_sem=halo_send_sems.at[i],
            recv_sem=halo_recv_sems.at[i],
            device_id=target,
            device_id_type=MESH,
        )
        halos.append((can_send, can_recv, copy))
    column_halos = halos[:2] + halos[2:6] + halos[10:14]
    row_halos = halos[6:10] + halos[14:18]

    pl.semaphore_wait(barrier, len(greeted))
    for can_send, _, copy in halos:
        when(can_send, copy.start)
    main_levels(SPLIT, lev_grp)
    main_lat(0)
    send_half(0)
    for load in panel_loads:
        load.start()
    for h in range(1, halves):
        main_levels(h * lev_grp, (h + 1) * lev_grp)
        main_lat(h)
        send_half(h)

    for _, can_recv, copy in column_halos:
        when(can_recv, copy.wait_recv)
    for i, (block, shift) in enumerate(((3, 2 * nk - 2), (0, 2 * nk + 2))):
        got = fold_recv[i]
        for part, tail in enumerate((got, turn(got, 2 * nk, 1))):
            cols[block, pl.ds(SUB + part * mid, mid)] = jnp.where(
                lane < 2 * nk, tail, turn(tail, shift, 1)
            )
    cye = cy + 2 * SUB
    row_e = iota((cye, 1), 0)
    kap_l = jnp.zeros((1, LANES), F32)
    factor_l = jnp.zeros((1, LANES), F32)
    lane_level = lax.div(lax.rem(lane, nk), EDGE)
    for l in range(levels):
        kap_l = jnp.where(lane_level == l, kappa_ref[l], kap_l)
        factor_l = jnp.where(lane_level == l, factor_of(l), factor_l)

    flags = {(dy, dx): ocean_of(dy, dx)[:, :LANES] for dy in (-1, 0, 1) for dx in (-1, 0, 1)}

    def coefficients(i, dx):
        block = cols[i]
        oc = jnp.where(
            row_e < SUB, flags[-1, dx], jnp.where(row_e < SUB + cy, flags[0, dx], flags[1, dx])
        )
        half = 0.5 * oc
        u = jnp.where(lane < nk, turn(block, -2 * nk, 1), turn(block, -nk, 1)) * half
        v = jnp.where(lane < nk, turn(block, -3 * nk, 1), turn(block, -2 * nk, 1)) * half
        return stencil(u, v, kap_l * oc)

    def step_left(left, right, coef):
        e = jnp.where(col == EDGE - 1, turn(right, EDGE - 1, 1), turn(left, -1, 1))
        return advance(left, e, turn(left, 1, 1), turn(left, -1, 0), turn(left, 1, 0), coef)

    def step_right(left, right, coef):
        w = jnp.where(col == 0, turn(left, 1 - EDGE, 1), turn(right, 1, 1))
        return advance(right, turn(right, -1, 1), w, turn(right, -1, 0), turn(right, 1, 0), coef)

    own = coefficients(1, 0)
    left1 = step_left(cols[0], cols[1], coefficients(0, -1))
    west1 = step_right(cols[0], cols[1], own)
    west2 = step_right(left1, west1, own)
    own = coefficients(2, 0)
    east1 = step_left(cols[2], cols[3], own)
    right1 = step_right(cols[2], cols[3], coefficients(3, 1))
    east2 = step_left(east1, right1, own)
    both1 = jnp.where(col < 2, west1, east1)[SUB : SUB + cy]
    both2 = jnp.where(col < 2, west2, east2)[SUB : SUB + cy]
    temp_salt, _, rho = mean_fields(
        both1, turn(both1, -nk, 1), both2, turn(both2, -nk, 1), factor_l
    )
    packed = jnp.where(
        lane < 2 * nk, temp_salt, jnp.where(lane < 3 * nk, turn(rho, 2 * nk, 1), 0.0)
    ).astype(BF16)
    narrow = n_gx * trows
    thin = jnp.dot(flat[:narrow], pick_c[:, :cy], preferred_element_type=F32)
    ei, ec = iota((narrow, cy), 0), iota((narrow, cy), 1)
    thin = jnp.where(lax.div(ec, srows) == lax.div(ei, trows), thin, 0.0).astype(BF16)
    edge_lat = jnp.dot(thin, packed, preferred_element_type=F32).astype(BF16)
    for g in range(n_gx):
        e_send[g] = edge_lat[g * trows : (g + 1) * trows]

    e_copies = []
    for d in order:
        target = partner(gx, d, n_gx)
        copy = pltpu.make_async_remote_copy(
            src_ref=e_send.at[target],
            dst_ref=e_recv.at[gx],
            send_sem=e_send_sems.at[d],
            recv_sem=e_recv_sems.at[d],
            device_id=(role, gy, target),
            device_id_type=MESH,
        )
        copy.start()
        e_copies.append(copy)
    e_recv[pl.ds(gx, 1)] = e_send[pl.ds(gx, 1)]

    for _, can_recv, copy in row_halos:
        when(can_recv, copy.wait_recv)
    sub8 = iota((SUB, 1), 0)
    ocean_below, ocean_above = ocean_of(-1, 0), ocean_of(1, 0)

    def up(a, b):
        return jnp.where(sub8 == SUB - 1, turn(b, -1, 0), turn(a, -1, 0))

    def down(a, b):
        return jnp.where(sub8 == 0, turn(a, 1, 0), turn(b, 1, 0))

    def rows_step(c, n, b, coef):
        return advance(c, turn(c, -1, 1), turn(c, 1, 1), n, b, coef)

    for l in range(levels):
        kap = kappa_ref[l] * ocean
        factor = factor_of(l)
        flow = [uv[i, l, pl.ds(0, 16)].astype(F32)[:SUB] * (0.5 * ocean) for i in range(2)]
        other = [halo_uv[0, i, l].astype(F32) * (0.5 * ocean_below) for i in range(2)]
        flow = stencil(*flow, kap)
        other = stencil(*other, kappa_ref[l] * ocean_below)
        ones, twos = [], []
        for t in range(2):
            far, edge, near = halo_x[0, t, l], x0[t, l, pl.ds(0, SUB)], x0[t, l, pl.ds(SUB, SUB)]
            out1 = rows_step(far, up(far, edge), turn(far, 1, 0), other)
            in1 = rows_step(edge, up(edge, near), down(far, edge), flow)
            ones.append(in1)
            next1 = x1[t, l, pl.ds(SUB, SUB)]
            twos.append(rows_step(in1, up(in1, next1), down(out1, in1), flow))
        for f, value in enumerate(mean_fields(*ones, *twos, factor)):
            means[f, l, pl.ds(0, SUB)] = value.astype(BF16)

        flow = [uv[i, l, pl.ds(cy - 16, 16)].astype(F32)[SUB:] * (0.5 * ocean) for i in range(2)]
        other = [halo_uv[1, i, l].astype(F32) * (0.5 * ocean_above) for i in range(2)]
        flow = stencil(*flow, kap)
        other = stencil(*other, kappa_ref[l] * ocean_above)
        ones, twos = [], []
        for t in range(2):
            far = halo_x[1, t, l]
            edge = x0[t, l, pl.ds(cy - SUB, SUB)]
            near = x0[t, l, pl.ds(cy - 2 * SUB, SUB)]
            out1 = rows_step(far, turn(far, -1, 0), down(edge, far), other)
            in1 = rows_step(edge, up(edge, far), down(near, edge), flow)
            ones.append(in1)
            next1 = x1[t, l, pl.ds(cy - 2 * SUB, SUB)]
            twos.append(rows_step(in1, up(in1, out1), down(next1, in1), flow))
        for f, value in enumerate(mean_fields(*ones, *twos, factor)):
            means[f, l, pl.ds(cy - SUB, SUB)] = value.astype(BF16)

    ends = jnp.concatenate([band[:lev_rows], band[out_r - lev_rows :]], axis=0)
    for h in range(halves):
        for f in range(3):
            rows = means[f, pl.ds(h * lev_grp, lev_grp)].reshape(in_r, cx)
            got = jnp.dot(ends, rows, preferred_element_type=F32)
            got = jnp.where(at_edge, 0.0, got).astype(BF16)
            stage(h, 0, f, got[:lev_rows])
            stage(h, n_gx - 1, f, got[lev_rows:])
        for d in order:
            target, copy = bulk(h, d)
            pl.when((target == 0) | (target == n_gx - 1))(copy.start)
        pl.when(at_end)(local(h).start)

    for d in order:
        target, copy = bulk(halves - 1, d)
        pl.when(held(target))(copy.start)

    depth = sw + LANES
    sub = iota((1, SUB, 1), 1)

    def tile_of(j):
        return lax.div(start_ref[j], LANES)

    blank = jnp.zeros((SUB, tb), F32)
    for j in range(nblk):
        panel_loads[j].wait()
        off = jnp.full((1, tb), start_ref[j] - tile_of(j) * LANES, jnp.int32)
        rows = panel[j].astype(F32)
        parts = [rows[i * SUB : (i + 1) * SUB] for i in range(sw // SUB)]
        bit = 1
        while bit < SUB:
            taken = lax.rem(lax.div(off, bit), 2) == 1
            low = sub8 < bit
            ring = [turn(part, bit, 0) for part in parts] + [blank]
            parts = [
                jnp.where(
                    taken,
                    jnp.where(low, ring[i - 1] if i else blank, ring[i]),
                    parts[i] if i < len(parts) else blank,
                )
                for i in range(len(ring))
            ] if bit == 1 else [
                jnp.where(taken, jnp.where(low, ring[i - 1] if i else blank, ring[i]), parts[i])
                for i in range(len(parts))
            ]
            bit *= 2
        step = 1
        while step * SUB < LANES:
            taken = lax.rem(lax.div(off, step * SUB), 2) == 1
            longer = len(parts) + step
            parts = [
                jnp.where(
                    taken,
                    parts[i - step] if i >= step else blank,
                    parts[i] if i < len(parts) else blank,
                )
                for i in range(longer)
            ]
            step *= 2
        assert len(parts) == depth // SUB
        shifted[j] = jnp.concatenate(parts, axis=0).astype(BF16)

    glanes = gather.shape[2]
    lanes = iota((1, glanes), 1)
    labels = lax.rem(lanes, groups)

    def add_area(r, so_far):
        return so_far + jnp.where(labels == cluster_ref[r], area_ref[r], 0.0)

    area_sum = lax.fori_loop(
        0, cluster_ref.shape[0], add_area, jnp.zeros((1, glanes), F32), unroll=8
    )
    thick_total = sum(1.0 + 0.25 * k for k in range(levels * n_role))
    denom = area_sum * (thick_total * nblk * tb)
    first_row = (gy * n_gx + gx) * trows
    out_rows = halves * half_rows
    orow = iota((out_rows, 1), 0)
    ti = lax.rem(orow, trows)
    hot = jnp.zeros((out_rows, glanes), F32)
    for t in range(trows):
        row_hot = jnp.where(labels == cluster_ref[first_row + t], area_ref[first_row + t], 0.0)
        hot = jnp.where(ti == t, row_hot, hot)
    olevel = lax.div(orow, half_rows) * lev_grp + lax.div(lax.rem(orow, lev_rows), trows)
    ofield = lax.div(lax.rem(orow, half_rows), lev_rows)
    thick = 1.0 + 0.25 * (level0 + olevel).astype(F32)
    field = lax.div(lanes, groups)
    hot = jnp.where(ofield == field, hot * thick, 0.0)

    pk, pc = iota((LANES, cx), 0), iota((LANES, cx), 1)
    place = jnp.where(pc < 2, pc, jnp.where(pc >= cx - 2, pc - (cx - EDGE), -1))
    place = (place == lax.rem(pk, EDGE)).astype(F32).astype(BF16)
    mine_q = ofield * levels + olevel
    for copy in e_copies:
        copy.wait_recv()
    for s in range(n_gx):
        block = e_recv[s].astype(F32)
        tall = jnp.concatenate([block] * (out_rows // trows), axis=0)
        tall = jnp.where(quad == mine_q, tall, 0.0).astype(BF16)
        put = jnp.dot(tall, place, preferred_element_type=F32).astype(BF16)
        for i in range(tiles):
            placed[s * tiles + i] = put[:, i * LANES : (i + 1) * LANES]

    weighted = []
    for h in range(halves):
        for d in order:
            bulk(h, d)[1].wait_recv()
        local(h).wait()
        rows = pl.ds(h * half_rows, half_rows)
        for i in range(n_gx * tiles):
            lat[h][i] = lat[h][i] + placed[i, rows]
        squares = jnp.zeros((half_rows, tb), F32)
        for j in range(nblk):
            tile = tile_of(j)
            window = jnp.concatenate([lat[h][tile + i] for i in range(depth // LANES)], axis=1)
            values = jnp.dot(window, shifted[j], preferred_element_type=F32)
            squares = squares + values * values
            result[rows, pl.ds(j * tb, tb)] = values
        weighted.append(jnp.sum(squares, axis=1, keepdims=True))
    weighted = jnp.concatenate(weighted, axis=0) * hot
    part = jnp.sum(weighted, axis=0, keepdims=True) / denom

    def for_others(do):
        if total <= 64:
            for d in range(1, total):
                do(peer(d))
        else:

            @pl.loop(1, total)
            def _(d):
                do(peer(d))

    def send(device):
        pltpu.make_async_remote_copy(
            src_ref=gather.at[me],
            dst_ref=gather.at[me],
            send_sem=sum_sems.at[0],
            recv_sem=sum_sems.at[1],
            device_id=device,
            device_id_type=MESH,
        ).start()

    gather[me] = part
    for_others(send)

    for h in range(halves):
        for f in range(3):
            for i in range(lev_grp):
                row = h * half_rows + f * lev_rows + i * trows
                out_ref[f, h * lev_grp + i] = result[pl.ds(row, trows), :].astype(BF16)

    for can_send, _, copy in halos:
        when(can_send, copy.wait_send)
    for h in range(halves):
        for d in order:
            bulk(h, d)[1].wait_send()
    for copy in e_copies:
        copy.wait_send()
    every = gather.at[pl.ds(0, total - 1)]
    for i in (1, 0):
        pltpu.make_async_copy(every, every, sum_sems.at[i]).wait()
    sums = jnp.sum(gather[...], axis=0)
    for f in range(3):
        sums_ref[pl.ds(f, 1), :] = turn(sums, -f * groups, 1)[:, :groups]


def store_kernel(remapped_ref, sums_ref, remapped_hbm, sums_hbm, sems):
    copies = [
        pltpu.make_async_copy(remapped_ref, remapped_hbm, sems.at[0]),
        pltpu.make_async_copy(sums_ref, sums_hbm, sems.at[1]),
    ]
    for copy in copies:
        copy.start()
    for copy in copies:
        copy.wait()


def body(
    dims,
    area,
    thermal_anomaly,
    saltiness_anomaly,
    zonal_flow_fraction,
    meridional_flow_fraction,
    mixing_coefficient,
    continent_patch_numbering,
    parallel_band_coefficients,
    meridian_panel_coefficients,
    panel_starting_source_meridian,
    target_parallel_cluster,
):
    n_role, n_gy, n_gx, levels, cy, cx, trows, srows, nblk, sw, tb, groups = dims
    total = n_role * n_gy * n_gx
    lev_grp = 16 // trows
    halves = levels // lev_grp
    half_rows = 3 * lev_grp * trows
    glanes = -(-3 * groups // LANES) * LANES
    hbm = pl.BlockSpec(memory_space=pltpu.MemorySpace.HBM)
    vmem = pl.BlockSpec(memory_space=pltpu.VMEM)
    brows = -(-n_gx * trows // LANES) * LANES
    dma = pltpu.SemaphoreType.DMA
    columns = n_gx * cx
    out_rows = halves * half_rows
    remapped, sums = pl.pallas_call(
        functools.partial(kernel, dims),
        out_shape=(
            jax.ShapeDtypeStruct((3, levels, trows, nblk * tb), BF16),
            jax.ShapeDtypeStruct((3, groups), F32),
        ),
        in_specs=[hbm] * 11,
        out_specs=(vmem, vmem),
        scratch_shapes=[
            pltpu.SMEM(mixing_coefficient.shape, F32),
            pltpu.SMEM(continent_patch_numbering.shape, jnp.int32),
            pltpu.SMEM(panel_starting_source_meridian.shape, jnp.int32),
            pltpu.SMEM(target_parallel_cluster.shape, jnp.int32),
            pltpu.SMEM(area.shape, F32),
            pltpu.VMEM(parallel_band_coefficients.shape, BF16),
            pltpu.VMEM((2, levels, cy, cx), F32),
            pltpu.VMEM((2, levels, cy, cx), F32),
            pltpu.VMEM((2, levels, cy, cx), BF16),
            pltpu.VMEM((3, levels, cy, cx), BF16),
            pltpu.VMEM((2, 2, levels, SUB, cx), F32),
            pltpu.VMEM((2, 2, levels, SUB, cx), BF16),
            pltpu.VMEM((4, cy + 2 * SUB, LANES), F32),
            pltpu.VMEM((2, cy // 2, LANES), F32),
            pltpu.VMEM((2, cy // 2, LANES), F32),
            pltpu.VMEM((2, 2 * levels * LANES, LANES), BF16),
            pltpu.VMEM((brows, LANES), F32),
            pltpu.VMEM((halves, n_gx, cx // LANES, half_rows, LANES), BF16),
            tuple(
                pltpu.VMEM((columns // LANES + 1, half_rows, LANES), BF16) for _ in range(halves)
            ),
            pltpu.VMEM((n_gx, trows, LANES), BF16),
            pltpu.VMEM((n_gx, trows, LANES), BF16),
            pltpu.VMEM((columns // LANES, out_rows, LANES), BF16),
            pltpu.VMEM((nblk, sw, tb), BF16),
            pltpu.VMEM((nblk, sw + LANES, tb), BF16),
            pltpu.VMEM((out_rows, nblk * tb), F32),
            pltpu.VMEM((total, 1, glanes), F32),
            dma((halves, 4)),
            dma((6,)),
            dma((nblk,)),
            dma((18,)),
            dma((18,)),
            dma((halves, n_gx)),
            dma((halves, n_gx)),
            dma((halves,)),
            dma((n_gx,)),
            dma((n_gx,)),
            dma((2,)),
        ],
        compiler_params=pltpu.CompilerParams(
            collective_id=0, has_side_effects=True, vmem_limit_bytes=26 * 1024 * 1024
        ),
        name="ocean",
    )(
        *(
            pltpu.with_memory_space_constraint(array, pltpu.MemorySpace.HBM)
            for array in (
                thermal_anomaly,
                saltiness_anomaly,
                zonal_flow_fraction,
                meridional_flow_fraction,
                meridian_panel_coefficients,
                mixing_coefficient,
                continent_patch_numbering,
                panel_starting_source_meridian,
                target_parallel_cluster,
                jnp.asarray(area),
                parallel_band_coefficients,
            )
        )
    )
    return pl.pallas_call(
        store_kernel,
        out_shape=(
            jax.ShapeDtypeStruct(remapped.shape, BF16),
            jax.ShapeDtypeStruct(sums.shape, F32),
        ),
        in_specs=[vmem, vmem],
        out_specs=(hbm, hbm),
        scratch_shapes=[dma((2,))],
        compiler_params=pltpu.CompilerParams(vmem_limit_bytes=4 * 1024 * 1024),
        name="store",
    )(remapped, sums)


def solution(mesh):
    in_specs = (
        P("role", "gy", "gx"),
        P("role", "gy", "gx"),
        P("role", "gy", "gx"),
        P("role", "gy", "gx"),
        P("role"),
        P(),
        P("gy", None, None),
        P(),
        P(),
        P(),
    )
    out_specs = (P(None, "role", ("gy", "gx"), None), P())

    def run(*args):
        n_role, n_gy, n_gx = (mesh.shape[a] for a in ("role", "gy", "gx"))
        levels, rows, cols = args[0].shape
        _, trows, srows = args[6].shape
        nblk, sw, tb = args[7].shape
        dims = (
            n_role,
            n_gy,
            n_gx,
            levels // n_role,
            rows // n_gy,
            cols // n_gx,
            trows,
            srows,
            nblk,
            sw,
            tb,
            4 * n_gy,
        )
        nrows = args[9].shape[0]
        r = np.arange(nrows, dtype=np.float64)
        area = np.cos((-75.0 + 150.0 * (r + 0.5) / nrows) * (math.pi / 180.0)).astype(np.float32)
        return jax.shard_map(
            functools.partial(body, dims, area),
            mesh=mesh,
            in_specs=in_specs,
            out_specs=out_specs,
            check_vma=False,
        )(*args)

    return run
```

```python
import functools
import math

import jax
import jax.numpy as jnp
import numpy as np
from jax import lax
from jax.experimental import pallas as pl
from jax.experimental.pallas import tpu as pltpu
from jax.sharding import PartitionSpec as P

LANES = 128
SUB = 8
EDGE = 4
SPLIT = 3
F32 = jnp.float32
BF16 = jnp.bfloat16
MESH = pl.DeviceIdType.MESH


def wrap(value, count):
    return jnp.where(value >= count, value - count, value)


def iota(shape, dim):
    return lax.broadcasted_iota(jnp.int32, shape, dim)


def turn(value, shift, axis):
    size = value.shape[axis]
    shift = shift % size
    return pltpu.roll(value, shift, axis) if shift else value


def partner(index, d, count):
    if count & (count - 1):
        return wrap(index + d, count)
    other = index
    for bit in range(count.bit_length() - 1):
        if d >> bit & 1:
            step = 1 << bit
            other = other + step - 2 * step * lax.rem(lax.div(index, step), 2)
    return other


def position():
    return tuple(lax.axis_index(a) for a in ("role", "gy", "gx"))


def peer_of(dims, d):
    n_role, n_gy, n_gx = dims[:3]
    role, gy, gx = position()
    dx, dyr = d % n_gx, d // n_gx
    dy, dr = dyr % n_gy, dyr // n_gy
    return (wrap(role + dr, n_role), wrap(gy + dy, n_gy), wrap(gx + dx, n_gx))


def kernel(
    dims,
    temp_hbm,
    salt_hbm,
    zonal_hbm,
    merid_hbm,
    panel_hbm,
    kappa_hbm,
    land_hbm,
    start_hbm,
    cluster_hbm,
    area_hbm,
    band_hbm,
    out_ref,
    sums_ref,
    kappa_ref,
    land_ref,
    start_ref,
    cluster_ref,
    area_ref,
    band_ref,
    x0,
    x1,
    uv,
    means,
    halo_x,
    halo_uv,
    cols,
    fold_send,
    fold_recv,
    chosen,
    band_rows,
    lat_send,
    lat,
    e_send,
    e_recv,
    placed,
    panel,
    shifted,
    result,
    gather,
    in_sems,
    small_sems,
    panel_sems,
    halo_send_sems,
    halo_recv_sems,
    a2a_send_sems,
    a2a_recv_sems,
    local_sems,
    e_send_sems,
    e_recv_sems,
    sum_sems,
):
    n_role, n_gy, n_gx, levels, cy, cx, trows, srows, nblk, sw, tb, groups = dims
    role, gy, gx = position()
    total = n_role * n_gy * n_gx
    me = (role * n_gy + gy) * n_gx + gx
    lev_grp = 16 // trows
    halves = levels // lev_grp
    lev_rows = lev_grp * trows
    half_rows = 3 * lev_rows
    nk = EDGE * levels
    peer = functools.partial(peer_of, dims)

    smalls = (
        (kappa_hbm, kappa_ref),
        (land_hbm, land_ref),
        (band_hbm, band_ref),
        (start_hbm, start_ref),
        (cluster_hbm, cluster_ref),
        (area_hbm, area_ref),
    )
    small_loads = [
        pltpu.make_async_copy(src, dst, small_sems.at[i]) for i, (src, dst) in enumerate(smalls)
    ]
    for load in small_loads:
        load.start()
    sources = ((temp_hbm, x0.at[0]), (salt_hbm, x0.at[1]), (zonal_hbm, uv.at[0]), (merid_hbm, uv.at[1]))
    loads = []
    for h in range(halves):
        part = pl.ds(h * lev_grp, lev_grp)
        loads.append(
            [
                pltpu.make_async_copy(src.at[part], dst.at[part], in_sems.at[h, i])
                for i, (src, dst) in enumerate(sources)
            ]
        )
        for load in loads[h]:
            load.start()
    panel_loads = [
        pltpu.make_async_copy(panel_hbm.at[j], panel.at[j], panel_sems.at[j]) for j in range(nblk)
    ]

    barrier = pltpu.get_barrier_semaphore()
    greeted = set(range(1, n_gx)) | {d * n_gx for d in range(1, n_role * n_gy)}
    for dy in {1, n_gy - 1}:
        for dx in {1, n_gx - 1}:
            greeted.add(dy * n_gx + dx)
    greeted = sorted(greeted)
    for d in greeted:
        pl.semaphore_signal(barrier, inc=1, device_id=peer(d), device_id_type=MESH)

    lane = iota((1, LANES), 1)
    quad = lax.div(lane, EDGE)
    col = lax.rem(lane, EDGE)
    has_below = gy > 0
    has_above = gy < n_gy - 1

    @pl.when(gy == 0)
    def _():
        halo_x[0] = jnp.zeros_like(halo_x[0])
        halo_uv[0] = jnp.zeros_like(halo_uv[0])
        for i in range(4):
            cols[i, pl.ds(0, SUB)] = jnp.zeros((SUB, LANES), F32)

    @pl.when(gy == n_gy - 1)
    def _():
        halo_x[1] = jnp.zeros_like(halo_x[1])
        halo_uv[1] = jnp.zeros_like(halo_uv[1])
        for i in range(4):
            cols[i, pl.ds(SUB + cy, SUB)] = jnp.zeros((SUB, LANES), F32)

    columns = n_gx * cx
    for h in range(halves):
        lat[h][columns // LANES] = jnp.zeros((half_rows, LANES), BF16)

    def ocean_of(dy, dx):
        ty = gy + dy
        tx = wrap(gx + dx + n_gx, n_gx)
        number = jnp.full((1, cx), ty * n_gx + tx, jnp.int32)
        flag = jnp.where((jnp.full((1, cx), ty, jnp.int32) >= 0) & (jnp.full((1, cx), ty, jnp.int32) < n_gy), 1.0, 0.0)
        for i in range(land_ref.shape[0]):
            flag = jnp.where(jnp.full((1, cx), land_ref[i], jnp.int32) == number, 0.0, flag)
        return flag

    for load in small_loads:
        load.wait()
    ocean = ocean_of(0, 0)

    chosen[...] = jnp.zeros_like(chosen)
    for q in range(2 * levels):
        for side, (base, top) in enumerate(((0, 0), (LANES - 16, LANES - EDGE))):
            ck, cl = iota((16, LANES), 0) + base, iota((16, LANES), 1)
            hit = (ck >= top) & (ck < top + EDGE) & (ck - top == cl - 2 * nk - EDGE * q)
            chosen[side, pl.ds(q * LANES + base, 16)] = jnp.where(hit, 1.0, 0.0).astype(BF16)
    band_rows[...] = jnp.zeros_like(band_rows)
    for g in range(n_gx):
        band_rows[pl.ds(g * trows, trows), pl.ds(0, srows)] = band_ref[g].astype(F32)
    brows = band_rows.shape[0]
    out_r, in_r = n_gx * lev_rows, lev_grp * cy
    flat = band_rows[...].astype(BF16)
    ri, rq = iota((out_r, brows), 0), iota((out_r, brows), 1)
    pick_r = (lax.div(ri, lev_rows) == lax.div(rq, trows)) & (
        lax.rem(ri, trows) == lax.rem(rq, trows)
    )
    spread = jnp.dot(pick_r.astype(F32).astype(BF16), flat, preferred_element_type=F32)
    cs, cc = iota((LANES, in_r), 0), iota((LANES, in_r), 1)
    pick_c = (lax.rem(lax.rem(cc, cy), srows) == cs).astype(F32).astype(BF16)
    spread = jnp.dot(spread.astype(BF16), pick_c, preferred_element_type=F32)
    ai, ac = iota((out_r, in_r), 0), iota((out_r, in_r), 1)
    keep = (lax.div(lax.rem(ai, lev_rows), trows) == lax.div(ac, cy)) & (
        lax.div(lax.rem(ac, cy), srows) == lax.div(ai, lev_rows)
    )
    band = jnp.where(keep, spread, 0.0).astype(BF16)

    level0 = role * levels

    def stencil(u, v, kap):
        return 1.0 - 4.0 * kap, kap - u, kap + u, kap - v, kap + v

    def advance(c, e, w, n, b, coef):
        own, to_e, to_w, to_n, to_b = coef
        return (own * c + (to_e * e + to_w * w)) + (to_n * n + to_b * b)

    def whole(c, coef):
        tiles_of = range(len(c))
        left = [turn(a, -1, 1) for a in c]
        right = [turn(a, 1, 1) for a in c]
        out = []
        for i in tiles_of:
            e = jnp.where(lane == LANES - 1, left[i + 1], left[i]) if i + 1 < len(c) else left[i]
            w = jnp.where(lane == 0, right[i - 1], right[i]) if i else right[i]
            out.append(advance(c[i], e, w, turn(c[i], -1, 0), turn(c[i], 1, 0), coef[i]))
        return out

    def mean_fields(t1, s1, t2, s2, factor):
        t, s = t1 + t2, s1 + s2
        rho = 0.39 * s - (0.5 * factor) * t - 0.01 * (t1 * t1 + t2 * t2)
        return 0.5 * t, 0.5 * s, rho

    def factor_of(l):
        return 0.17 * (1.0 + 0.03 * (level0 + l).astype(F32))

    flag0 = ocean[:, :LANES]
    half0 = 0.5 * flag0
    wide = iota((1, cx), 1)
    at_edge = (wide < 2) | (wide >= cx - 2)
    tiles = cx // LANES
    order = list(range(n_gx - 1, 0, -1))
    at_end = (gx == 0) | (gx == n_gx - 1)

    def bulk(h, d):
        target = partner(gx, d, n_gx)
        return target, pltpu.make_async_remote_copy(
            src_ref=lat_send.at[h, target],
            dst_ref=lat[h].at[pl.ds(gx * tiles, tiles)],
            send_sem=a2a_send_sems.at[h, d],
            recv_sem=a2a_recv_sems.at[h, d],
            device_id=(role, gy, target),
            device_id_type=MESH,
        )

    def local(h):
        return pltpu.make_async_copy(
            lat_send.at[h, gx],
            lat[h].at[pl.ds(gx * tiles, tiles)],
            local_sems.at[h],
        )

    def stage(h, g, f, rows):
        for i in range(tiles):
            lat_send[h, g, i, pl.ds(f * lev_rows, lev_rows)] = rows[
                :, i * LANES : (i + 1) * LANES
            ]

    def main_levels(first_level, last_level):
        for l in range(first_level, last_level):
            kap = kappa_ref[l] * flag0
            spans = [pl.ds(i * LANES, LANES) for i in range(tiles)]
            coef = [
                stencil(
                    uv[0, l, :, span].astype(F32) * half0, uv[1, l, :, span].astype(F32) * half0, kap
                )
                for span in spans
            ]
            one = [whole([x0[t, l, :, span] for span in spans], coef) for t in range(2)]
            two = [whole(one[t], coef) for t in range(2)]
            factor = factor_of(l)
            for i, span in enumerate(spans):
                x1[0, l, :, span] = one[0][i]
                x1[1, l, :, span] = one[1][i]
                fields = mean_fields(one[0][i], one[1][i], two[0][i], two[1][i], factor)
                for f in range(3):
                    means[f, l, :, span] = fields[f].astype(BF16)

    def main_lat(h):
        for f in range(3):
            rows = means[f, pl.ds(h * lev_grp, lev_grp)].reshape(in_r, cx)
            got = jnp.dot(band[lev_rows : out_r - lev_rows], rows, preferred_element_type=F32)
            got = jnp.where(at_edge, 0.0, got).astype(BF16)
            for g in range(1, n_gx - 1):
                stage(h, g, f, got[(g - 1) * lev_rows : g * lev_rows])

    def held(target):
        return (target == n_gx // 2 - 1) | (target == n_gx // 2)

    def send_half(h):
        for d in order:
            target, copy = bulk(h, d)
            now = (target > 0) & (target < n_gx - 1)
            if h == halves - 1:
                now = now & jnp.logical_not(held(target))
            pl.when(now)(copy.start)
        pl.when(jnp.logical_not(at_end))(local(h).start)

    for load in loads[0]:
        load.wait()
    main_levels(0, SPLIT)
    for later in loads[1:]:
        for load in later:
            load.wait()
    packed = []
    for side, edge in enumerate((pl.ds(0, LANES), pl.ds(cx - LANES, LANES))):
        block = jnp.concatenate(
            [uv[q // levels, q % levels, :, edge] for q in range(2 * levels)], axis=1
        )
        block = jnp.dot(block, chosen[side], preferred_element_type=F32)
        for q in range(2 * levels):
            tile = x0[q // levels, q % levels, :, edge]
            block = jnp.where(quad == q, turn(tile, EDGE * (q + side), 1), block)
        packed.append(block)
    first, last = packed
    cols[1, pl.ds(SUB, cy)] = first
    cols[2, pl.ds(SUB, cy)] = last
    mid = cy // 2

    def fold(block):
        return jnp.where(lane < 2 * nk, block[:mid], turn(block[mid:], 2 * nk, 1))

    fold_send[0] = fold(jnp.where(col < 2, first, turn(first, 2 - 2 * nk, 1)))
    fold_send[1] = fold(jnp.where(col < 2, turn(last, -2 - 2 * nk, 1), last))

    west = wrap(gx + n_gx - 1, n_gx)
    east = wrap(gx + 1, n_gx)
    plan = [
        (None, None, fold_send.at[0], fold_recv.at[0], (role, gy, west)),
        (None, None, fold_send.at[1], fold_recv.at[1], (role, gy, east)),
    ]
    for side, (can_send, can_recv) in enumerate(((has_below, has_above), (has_above, has_below))):
        ty = gy - 1 if side == 0 else gy + 1
        mine = SUB if side == 0 else cy
        theirs = SUB + cy if side == 0 else 0
        for block, there, tx in ((1, 1, gx), (2, 2, gx), (1, 3, west), (2, 0, east)):
            plan.append(
                (
                    can_send,
                    can_recv,
                    cols.at[block, pl.ds(mine, SUB)],
                    cols.at[there, pl.ds(theirs, SUB)],
                    (role, ty, tx),
                )
            )
        row = 0 if side == 0 else cy - 2
        slot = 0 if side == 0 else SUB - 2
        for t, ref in enumerate((temp_hbm, salt_hbm)):
            plan.append(
                (
                    can_send,
                    can_recv,
                    ref.at[:, pl.ds(row, 2), :],
                    halo_x.at[1 - side, t, :, pl.ds(slot, 2), :],
                    (role, ty, gx),
                )
            )
        row = 0 if side == 0 else cy - SUB
        for t, ref in enumerate((zonal_hbm, merid_hbm)):
            plan.append(
                (
                    can_send,
                    can_recv,
                    ref.at[:, pl.ds(row, SUB), :],
                    halo_uv.at[1 - side, t],
                    (role, ty, gx),
                )
            )

    def when(cond, do):
        if cond is None:
            do()
        else:
            pl.when(cond)(do)

    halos = []
    for i, (can_send, can_recv, src, dst, target) in enumerate(plan):
        copy = pltpu.make_async_remote_copy(
            src_ref=src,
            dst_ref=dst,
            send_sem=halo_send_sems.at[i],
            recv_sem=halo_recv_sems.at[i],
            device_id=target,
            device_id_type=MESH,
        )
        halos.append((can_send, can_recv, copy))
    column_halos = halos[:2] + halos[2:6] + halos[10:14]
    row_halos = halos[6:10] + halos[14:18]

    pl.semaphore_wait(barrier, len(greeted))
    for can_send, _, copy in halos:
        when(can_send, copy.start)
    main_levels(SPLIT, lev_grp)
    main_lat(0)
    send_half(0)
    for load in panel_loads:
        load.start()
    for h in range(1, halves):
        main_levels(h * lev_grp, (h + 1) * lev_grp)
        main_lat(h)
        send_half(h)

    for _, can_recv, copy in column_halos:
        when(can_recv, copy.wait_recv)
    for i, (block, shift) in enumerate(((3, 2 * nk - 2), (0, 2 * nk + 2))):
        got = fold_recv[i]
        for part, tail in enumerate((got, turn(got, 2 * nk, 1))):
            cols[block, pl.ds(SUB + part * mid, mid)] = jnp.where(
                lane < 2 * nk, tail, turn(tail, shift, 1)
            )
    cye = cy + 2 * SUB
    row_e = iota((cye, 1), 0)
    kap_l = jnp.zeros((1, LANES), F32)
    factor_l = jnp.zeros((1, LANES), F32)
    lane_level = lax.div(lax.rem(lane, nk), EDGE)
    for l in range(levels):
        kap_l = jnp.where(lane_level == l, kappa_ref[l], kap_l)
        factor_l = jnp.where(lane_level == l, factor_of(l), factor_l)

    flags = {(dy, dx): ocean_of(dy, dx)[:, :LANES] for dy in (-1, 0, 1) for dx in (-1, 0, 1)}

    def coefficients(i, dx):
        block = cols[i]
        oc = jnp.where(
            row_e < SUB, flags[-1, dx], jnp.where(row_e < SUB + cy, flags[0, dx], flags[1, dx])
        )
        half = 0.5 * oc
        u = jnp.where(lane < nk, turn(block, -2 * nk, 1), turn(block, -nk, 1)) * half
        v = jnp.where(lane < nk, turn(block, -3 * nk, 1), turn(block, -2 * nk, 1)) * half
        return stencil(u, v, kap_l * oc)

    def step_left(left, right, coef):
        e = jnp.where(col == EDGE - 1, turn(right, EDGE - 1, 1), turn(left, -1, 1))
        return advance(left, e, turn(left, 1, 1), turn(left, -1, 0), turn(left, 1, 0), coef)

    def step_right(left, right, coef):
        w = jnp.where(col == 0, turn(left, 1 - EDGE, 1), turn(right, 1, 1))
        return advance(right, turn(right, -1, 1), w, turn(right, -1, 0), turn(right, 1, 0), coef)

    own = coefficients(1, 0)
    left1 = step_left(cols[0], cols[1], coefficients(0, -1))
    west1 = step_right(cols[0], cols[1], own)
    west2 = step_right(left1, west1, own)
    own = coefficients(2, 0)
    east1 = step_left(cols[2], cols[3], own)
    right1 = step_right(cols[2], cols[3], coefficients(3, 1))
    east2 = step_left(east1, right1, own)
    both1 = jnp.where(col < 2, west1, east1)[SUB : SUB + cy]
    both2 = jnp.where(col < 2, west2, east2)[SUB : SUB + cy]
    temp_salt, _, rho = mean_fields(
        both1, turn(both1, -nk, 1), both2, turn(both2, -nk, 1), factor_l
    )
    packed = jnp.where(
        lane < 2 * nk, temp_salt, jnp.where(lane < 3 * nk, turn(rho, 2 * nk, 1), 0.0)
    ).astype(BF16)
    narrow = n_gx * trows
    thin = jnp.dot(flat[:narrow], pick_c[:, :cy], preferred_element_type=F32)
    ei, ec = iota((narrow, cy), 0), iota((narrow, cy), 1)
    thin = jnp.where(lax.div(ec, srows) == lax.div(ei, trows), thin, 0.0).astype(BF16)
    edge_lat = jnp.dot(thin, packed, preferred_element_type=F32).astype(BF16)
    for g in range(n_gx):
        e_send[g] = edge_lat[g * trows : (g + 1) * trows]

    e_copies = []
    for d in order:
        target = partner(gx, d, n_gx)
        copy = pltpu.make_async_remote_copy(
            src_ref=e_send.at[target],
            dst_ref=e_recv.at[gx],
            send_sem=e_send_sems.at[d],
            recv_sem=e_recv_sems.at[d],
            device_id=(role, gy, target),
            device_id_type=MESH,
        )
        copy.start()
        e_copies.append(copy)
    e_recv[pl.ds(gx, 1)] = e_send[pl.ds(gx, 1)]

    for _, can_recv, copy in row_halos:
        when(can_recv, copy.wait_recv)
    sub8 = iota((SUB, 1), 0)
    ocean_below, ocean_above = ocean_of(-1, 0), ocean_of(1, 0)

    def up(a, b):
        return jnp.where(sub8 == SUB - 1, turn(b, -1, 0), turn(a, -1, 0))

    def down(a, b):
        return jnp.where(sub8 == 0, turn(a, 1, 0), turn(b, 1, 0))

    def rows_step(c, n, b, coef):
        return advance(c, turn(c, -1, 1), turn(c, 1, 1), n, b, coef)

    for l in range(levels):
        kap = kappa_ref[l] * ocean
        factor = factor_of(l)
        flow = [uv[i, l, pl.ds(0, 16)].astype(F32)[:SUB] * (0.5 * ocean) for i in range(2)]
        other = [halo_uv[0, i, l].astype(F32) * (0.5 * ocean_below) for i in range(2)]
        flow = stencil(*flow, kap)
        other = stencil(*other, kappa_ref[l] * ocean_below)
        ones, twos = [], []
        for t in range(2):
            far, edge, near = halo_x[0, t, l], x0[t, l, pl.ds(0, SUB)], x0[t, l, pl.ds(SUB, SUB)]
            out1 = rows_step(far, up(far, edge), turn(far, 1, 0), other)
            in1 = rows_step(edge, up(edge, near), down(far, edge), flow)
            ones.append(in1)
            next1 = x1[t, l, pl.ds(SUB, SUB)]
            twos.append(rows_step(in1, up(in1, next1), down(out1, in1), flow))
        for f, value in enumerate(mean_fields(*ones, *twos, factor)):
            means[f, l, pl.ds(0, SUB)] = value.astype(BF16)

        flow = [uv[i, l, pl.ds(cy - 16, 16)].astype(F32)[SUB:] * (0.5 * ocean) for i in range(2)]
        other = [halo_uv[1, i, l].astype(F32) * (0.5 * ocean_above) for i in range(2)]
        flow = stencil(*flow, kap)
        other = stencil(*other, kappa_ref[l] * ocean_above)
        ones, twos = [], []
        for t in range(2):
            far = halo_x[1, t, l]
            edge = x0[t, l, pl.ds(cy - SUB, SUB)]
            near = x0[t, l, pl.ds(cy - 2 * SUB, SUB)]
            out1 = rows_step(far, turn(far, -1, 0), down(edge, far), other)
            in1 = rows_step(edge, up(edge, far), down(near, edge), flow)
            ones.append(in1)
            next1 = x1[t, l, pl.ds(cy - 2 * SUB, SUB)]
            twos.append(rows_step(in1, up(in1, out1), down(next1, in1), flow))
        for f, value in enumerate(mean_fields(*ones, *twos, factor)):
            means[f, l, pl.ds(cy - SUB, SUB)] = value.astype(BF16)

    ends = jnp.concatenate([band[:lev_rows], band[out_r - lev_rows :]], axis=0)
    for h in range(halves):
        for f in range(3):
            rows = means[f, pl.ds(h * lev_grp, lev_grp)].reshape(in_r, cx)
            got = jnp.dot(ends, rows, preferred_element_type=F32)
            got = jnp.where(at_edge, 0.0, got).astype(BF16)
            stage(h, 0, f, got[:lev_rows])
            stage(h, n_gx - 1, f, got[lev_rows:])
        pl.when(at_end)(local(h).start)
    for d in order:
        for h in range(halves):
            target, copy = bulk(h, d)
            pl.when((target == 0) | (target == n_gx - 1))(copy.start)

    for d in order:
        target, copy = bulk(halves - 1, d)
        pl.when(held(target))(copy.start)

    depth = sw + LANES
    sub = iota((1, SUB, 1), 1)

    def tile_of(j):
        return lax.div(start_ref[j], LANES)

    blank = jnp.zeros((SUB, tb), F32)
    for j in range(nblk):
        panel_loads[j].wait()
        off = jnp.full((1, tb), start_ref[j] - tile_of(j) * LANES, jnp.int32)
        rows = panel[j].astype(F32)
        parts = [rows[i * SUB : (i + 1) * SUB] for i in range(sw // SUB)]
        bit = 1
        while bit < SUB:
            taken = lax.rem(lax.div(off, bit), 2) == 1
            low = sub8 < bit
            ring = [turn(part, bit, 0) for part in parts] + [blank]
            parts = [
                jnp.where(
                    taken,
                    jnp.where(low, ring[i - 1] if i else blank, ring[i]),
                    parts[i] if i < len(parts) else blank,
                )
                for i in range(len(ring))
            ] if bit == 1 else [
                jnp.where(taken, jnp.where(low, ring[i - 1] if i else blank, ring[i]), parts[i])
                for i in range(len(parts))
            ]
            bit *= 2
        step = 1
        while step * SUB < LANES:
            taken = lax.rem(lax.div(off, step * SUB), 2) == 1
            longer = len(parts) + step
            parts = [
                jnp.where(
                    taken,
                    parts[i - step] if i >= step else blank,
                    parts[i] if i < len(parts) else blank,
                )
                for i in range(longer)
            ]
            step *= 2
        assert len(parts) == depth // SUB
        shifted[j] = jnp.concatenate(parts, axis=0).astype(BF16)

    glanes = gather.shape[2]
    lanes = iota((1, glanes), 1)
    labels = lax.rem(lanes, groups)

    def add_area(r, so_far):
        return so_far + jnp.where(labels == cluster_ref[r], area_ref[r], 0.0)

    area_sum = lax.fori_loop(
        0, cluster_ref.shape[0], add_area, jnp.zeros((1, glanes), F32), unroll=8
    )
    thick_total = sum(1.0 + 0.25 * k for k in range(levels * n_role))
    denom = area_sum * (thick_total * nblk * tb)
    first_row = (gy * n_gx + gx) * trows
    out_rows = halves * half_rows
    orow = iota((out_rows, 1), 0)
    ti = lax.rem(orow, trows)
    hot = jnp.zeros((out_rows, glanes), F32)
    for t in range(trows):
        row_hot = jnp.where(labels == cluster_ref[first_row + t], area_ref[first_row + t], 0.0)
        hot = jnp.where(ti == t, row_hot, hot)
    olevel = lax.div(orow, half_rows) * lev_grp + lax.div(lax.rem(orow, lev_rows), trows)
    ofield = lax.div(lax.rem(orow, half_rows), lev_rows)
    thick = 1.0 + 0.25 * (level0 + olevel).astype(F32)
    field = lax.div(lanes, groups)
    hot = jnp.where(ofield == field, hot * thick, 0.0)

    pk, pc = iota((LANES, cx), 0), iota((LANES, cx), 1)
    place = jnp.where(pc < 2, pc, jnp.where(pc >= cx - 2, pc - (cx - EDGE), -1))
    place = (place == lax.rem(pk, EDGE)).astype(F32).astype(BF16)
    mine_q = ofield * levels + olevel
    for copy in e_copies:
        copy.wait_recv()
    for s in range(n_gx):
        block = e_recv[s].astype(F32)
        tall = jnp.concatenate([block] * (out_rows // trows), axis=0)
        tall = jnp.where(quad == mine_q, tall, 0.0).astype(BF16)
        put = jnp.dot(tall, place, preferred_element_type=F32).astype(BF16)
        for i in range(tiles):
            placed[s * tiles + i] = put[:, i * LANES : (i + 1) * LANES]

    weighted = []
    for h in range(halves):
        for d in order:
            bulk(h, d)[1].wait_recv()
        local(h).wait()
        rows = pl.ds(h * half_rows, half_rows)
        for i in range(n_gx * tiles):
            lat[h][i] = lat[h][i] + placed[i, rows]
        squares = jnp.zeros((half_rows, tb), F32)
        for j in range(nblk):
            tile = tile_of(j)
            window = jnp.concatenate([lat[h][tile + i] for i in range(depth // LANES)], axis=1)
            values = jnp.dot(window, shifted[j], preferred_element_type=F32)
            squares = squares + values * values
            result[rows, pl.ds(j * tb, tb)] = values
        weighted.append(jnp.sum(squares, axis=1, keepdims=True))
    weighted = jnp.concatenate(weighted, axis=0) * hot
    part = jnp.sum(weighted, axis=0, keepdims=True) / denom

    def for_others(do):
        if total <= 64:
            for d in range(1, total):
                do(peer(d))
        else:

            @pl.loop(1, total)
            def _(d):
                do(peer(d))

    def send(device):
        pltpu.make_async_remote_copy(
            src_ref=gather.at[me],
            dst_ref=gather.at[me],
            send_sem=sum_sems.at[0],
            recv_sem=sum_sems.at[1],
            device_id=device,
            device_id_type=MESH,
        ).start()

    gather[me] = part
    for_others(send)

    for h in range(halves):
        for f in range(3):
            for i in range(lev_grp):
                row = h * half_rows + f * lev_rows + i * trows
                out_ref[f, h * lev_grp + i] = result[pl.ds(row, trows), :].astype(BF16)

    for can_send, _, copy in halos:
        when(can_send, copy.wait_send)
    for h in range(halves):
        for d in order:
            bulk(h, d)[1].wait_send()
    for copy in e_copies:
        copy.wait_send()
    every = gather.at[pl.ds(0, total - 1)]
    for i in (1, 0):
        pltpu.make_async_copy(every, every, sum_sems.at[i]).wait()
    sums = jnp.sum(gather[...], axis=0)
    for f in range(3):
        sums_ref[pl.ds(f, 1), :] = turn(sums, -f * groups, 1)[:, :groups]


def store_kernel(remapped_ref, sums_ref, remapped_hbm, sums_hbm, sems):
    copies = [
        pltpu.make_async_copy(remapped_ref, remapped_hbm, sems.at[0]),
        pltpu.make_async_copy(sums_ref, sums_hbm, sems.at[1]),
    ]
    for copy in copies:
        copy.start()
    for copy in copies:
        copy.wait()


def body(
    dims,
    area,
    thermal_anomaly,
    saltiness_anomaly,
    zonal_flow_fraction,
    meridional_flow_fraction,
    mixing_coefficient,
    continent_patch_numbering,
    parallel_band_coefficients,
    meridian_panel_coefficients,
    panel_starting_source_meridian,
    target_parallel_cluster,
):
    n_role, n_gy, n_gx, levels, cy, cx, trows, srows, nblk, sw, tb, groups = dims
    total = n_role * n_gy * n_gx
    lev_grp = 16 // trows
    halves = levels // lev_grp
    half_rows = 3 * lev_grp * trows
    glanes = -(-3 * groups // LANES) * LANES
    hbm = pl.BlockSpec(memory_space=pltpu.MemorySpace.HBM)
    vmem = pl.BlockSpec(memory_space=pltpu.VMEM)
    brows = -(-n_gx * trows // LANES) * LANES
    dma = pltpu.SemaphoreType.DMA
    columns = n_gx * cx
    out_rows = halves * half_rows
    remapped, sums = pl.pallas_call(
        functools.partial(kernel, dims),
        out_shape=(
            jax.ShapeDtypeStruct((3, levels, trows, nblk * tb), BF16),
            jax.ShapeDtypeStruct((3, groups), F32),
        ),
        in_specs=[hbm] * 11,
        out_specs=(vmem, vmem),
        scratch_shapes=[
            pltpu.SMEM(mixing_coefficient.shape, F32),
            pltpu.SMEM(continent_patch_numbering.shape, jnp.int32),
            pltpu.SMEM(panel_starting_source_meridian.shape, jnp.int32),
            pltpu.SMEM(target_parallel_cluster.shape, jnp.int32),
            pltpu.SMEM(area.shape, F32),
            pltpu.VMEM(parallel_band_coefficients.shape, BF16),
            pltpu.VMEM((2, levels, cy, cx), F32),
            pltpu.VMEM((2, levels, cy, cx), F32),
            pltpu.VMEM((2, levels, cy, cx), BF16),
            pltpu.VMEM((3, levels, cy, cx), BF16),
            pltpu.VMEM((2, 2, levels, SUB, cx), F32),
            pltpu.VMEM((2, 2, levels, SUB, cx), BF16),
            pltpu.VMEM((4, cy + 2 * SUB, LANES), F32),
            pltpu.VMEM((2, cy // 2, LANES), F32),
            pltpu.VMEM((2, cy // 2, LANES), F32),
            pltpu.VMEM((2, 2 * levels * LANES, LANES), BF16),
            pltpu.VMEM((brows, LANES), F32),
            pltpu.VMEM((halves, n_gx, cx // LANES, half_rows, LANES), BF16),
            tuple(
                pltpu.VMEM((columns // LANES + 1, half_rows, LANES), BF16) for _ in range(halves)
            ),
            pltpu.VMEM((n_gx, trows, LANES), BF16),
            pltpu.VMEM((n_gx, trows, LANES), BF16),
            pltpu.VMEM((columns // LANES, out_rows, LANES), BF16),
            pltpu.VMEM((nblk, sw, tb), BF16),
            pltpu.VMEM((nblk, sw + LANES, tb), BF16),
            pltpu.VMEM((out_rows, nblk * tb), F32),
            pltpu.VMEM((total, 1, glanes), F32),
            dma((halves, 4)),
            dma((6,)),
            dma((nblk,)),
            dma((18,)),
            dma((18,)),
            dma((halves, n_gx)),
            dma((halves, n_gx)),
            dma((halves,)),
            dma((n_gx,)),
            dma((n_gx,)),
            dma((2,)),
        ],
        compiler_params=pltpu.CompilerParams(
            collective_id=0, has_side_effects=True, vmem_limit_bytes=26 * 1024 * 1024
        ),
        name="ocean",
    )(
        *(
            pltpu.with_memory_space_constraint(array, pltpu.MemorySpace.HBM)
            for array in (
                thermal_anomaly,
                saltiness_anomaly,
                zonal_flow_fraction,
                meridional_flow_fraction,
                meridian_panel_coefficients,
                mixing_coefficient,
                continent_patch_numbering,
                panel_starting_source_meridian,
                target_parallel_cluster,
                jnp.asarray(area),
                parallel_band_coefficients,
            )
        )
    )
    return pl.pallas_call(
        store_kernel,
        out_shape=(
            jax.ShapeDtypeStruct(remapped.shape, BF16),
            jax.ShapeDtypeStruct(sums.shape, F32),
        ),
        in_specs=[vmem, vmem],
        out_specs=(hbm, hbm),
        scratch_shapes=[dma((2,))],
        compiler_params=pltpu.CompilerParams(vmem_limit_bytes=4 * 1024 * 1024),
        name="store",
    )(remapped, sums)


def solution(mesh):
    in_specs = (
        P("role", "gy", "gx"),
        P("role", "gy", "gx"),
        P("role", "gy", "gx"),
        P("role", "gy", "gx"),
        P("role"),
        P(),
        P("gy", None, None),
        P(),
        P(),
        P(),
    )
    out_specs = (P(None, "role", ("gy", "gx"), None), P())

    def run(*args):
        n_role, n_gy, n_gx = (mesh.shape[a] for a in ("role", "gy", "gx"))
        levels, rows, cols = args[0].shape
        _, trows, srows = args[6].shape
        nblk, sw, tb = args[7].shape
        dims = (
            n_role,
            n_gy,
            n_gx,
            levels // n_role,
            rows // n_gy,
            cols // n_gx,
            trows,
            srows,
            nblk,
            sw,
            tb,
            4 * n_gy,
        )
        nrows = args[9].shape[0]
        r = np.arange(nrows, dtype=np.float64)
        area = np.cos((-75.0 + 150.0 * (r + 0.5) / nrows) * (math.pi / 180.0)).astype(np.float32)
        return jax.shard_map(
            functools.partial(body, dims, area),
            mesh=mesh,
            in_specs=in_specs,
            out_specs=out_specs,
            check_vma=False,
        )(*args)

    return run
```

```python
import functools
import math

import jax
import jax.numpy as jnp
import numpy as np
from jax import lax
from jax.experimental import pallas as pl
from jax.experimental.pallas import tpu as pltpu
from jax.sharding import PartitionSpec as P

LANES = 128
SUB = 8
EDGE = 4
SPLIT = 3
F32 = jnp.float32
BF16 = jnp.bfloat16
MESH = pl.DeviceIdType.MESH


def wrap(value, count):
    return jnp.where(value >= count, value - count, value)


def iota(shape, dim):
    return lax.broadcasted_iota(jnp.int32, shape, dim)


def turn(value, shift, axis):
    size = value.shape[axis]
    shift = shift % size
    return pltpu.roll(value, shift, axis) if shift else value


def partner(index, d, count):
    if count & (count - 1):
        return wrap(index + d, count)
    other = index
    for bit in range(count.bit_length() - 1):
        if d >> bit & 1:
            step = 1 << bit
            other = other + step - 2 * step * lax.rem(lax.div(index, step), 2)
    return other


def position():
    return tuple(lax.axis_index(a) for a in ("role", "gy", "gx"))


def peer_of(dims, d):
    n_role, n_gy, n_gx = dims[:3]
    role, gy, gx = position()
    dx, dyr = d % n_gx, d // n_gx
    dy, dr = dyr % n_gy, dyr // n_gy
    return (wrap(role + dr, n_role), wrap(gy + dy, n_gy), wrap(gx + dx, n_gx))


def kernel(
    dims,
    temp_hbm,
    salt_hbm,
    zonal_hbm,
    merid_hbm,
    panel_hbm,
    kappa_hbm,
    land_hbm,
    start_hbm,
    cluster_hbm,
    area_hbm,
    band_hbm,
    out_ref,
    sums_ref,
    kappa_ref,
    land_ref,
    start_ref,
    cluster_ref,
    area_ref,
    band_ref,
    x0,
    x1,
    uv,
    means,
    halo_x,
    halo_uv,
    cols,
    fold_send,
    fold_recv,
    chosen,
    band_rows,
    lat_send,
    lat,
    e_send,
    e_recv,
    placed,
    panel,
    shifted,
    result,
    gather,
    in_sems,
    small_sems,
    panel_sems,
    halo_send_sems,
    halo_recv_sems,
    a2a_send_sems,
    a2a_recv_sems,
    local_sems,
    e_send_sems,
    e_recv_sems,
    sum_sems,
):
    n_role, n_gy, n_gx, levels, cy, cx, trows, srows, nblk, sw, tb, groups = dims
    role, gy, gx = position()
    total = n_role * n_gy * n_gx
    me = (role * n_gy + gy) * n_gx + gx
    lev_grp = 16 // trows
    halves = levels // lev_grp
    lev_rows = lev_grp * trows
    half_rows = 3 * lev_rows
    nk = EDGE * levels
    peer = functools.partial(peer_of, dims)

    smalls = (
        (kappa_hbm, kappa_ref),
        (land_hbm, land_ref),
        (band_hbm, band_ref),
        (start_hbm, start_ref),
        (cluster_hbm, cluster_ref),
        (area_hbm, area_ref),
    )
    small_loads = [
        pltpu.make_async_copy(src, dst, small_sems.at[i]) for i, (src, dst) in enumerate(smalls)
    ]
    for load in small_loads:
        load.start()
    sources = ((temp_hbm, x0.at[0]), (salt_hbm, x0.at[1]), (zonal_hbm, uv.at[0]), (merid_hbm, uv.at[1]))
    loads = []
    for h in range(halves):
        part = pl.ds(h * lev_grp, lev_grp)
        loads.append(
            [
                pltpu.make_async_copy(src.at[part], dst.at[part], in_sems.at[h, i])
                for i, (src, dst) in enumerate(sources)
            ]
        )
        for load in loads[h]:
            load.start()
    panel_loads = [
        pltpu.make_async_copy(panel_hbm.at[j], panel.at[j], panel_sems.at[j]) for j in range(nblk)
    ]

    barrier = pltpu.get_barrier_semaphore()
    greeted = set(range(1, n_gx)) | {d * n_gx for d in range(1, n_role * n_gy)}
    for dy in {1, n_gy - 1}:
        for dx in {1, n_gx - 1}:
            greeted.add(dy * n_gx + dx)
    greeted = sorted(greeted)
    for d in greeted:
        pl.semaphore_signal(barrier, inc=1, device_id=peer(d), device_id_type=MESH)

    lane = iota((1, LANES), 1)
    quad = lax.div(lane, EDGE)
    col = lax.rem(lane, EDGE)
    has_below = gy > 0
    has_above = gy < n_gy - 1

    @pl.when(gy == 0)
    def _():
        halo_x[0] = jnp.zeros_like(halo_x[0])
        halo_uv[0] = jnp.zeros_like(halo_uv[0])
        for i in range(4):
            cols[i, pl.ds(0, SUB)] = jnp.zeros((SUB, LANES), F32)

    @pl.when(gy == n_gy - 1)
    def _():
        halo_x[1] = jnp.zeros_like(halo_x[1])
        halo_uv[1] = jnp.zeros_like(halo_uv[1])
        for i in range(4):
            cols[i, pl.ds(SUB + cy, SUB)] = jnp.zeros((SUB, LANES), F32)

    columns = n_gx * cx
    for h in range(halves):
        lat[h][columns // LANES] = jnp.zeros((half_rows, LANES), BF16)

    def ocean_of(dy, dx):
        ty = gy + dy
        tx = wrap(gx + dx + n_gx, n_gx)
        number = jnp.full((1, cx), ty * n_gx + tx, jnp.int32)
        flag = jnp.where((jnp.full((1, cx), ty, jnp.int32) >= 0) & (jnp.full((1, cx), ty, jnp.int32) < n_gy), 1.0, 0.0)
        for i in range(land_ref.shape[0]):
            flag = jnp.where(jnp.full((1, cx), land_ref[i], jnp.int32) == number, 0.0, flag)
        return flag

    for load in small_loads:
        load.wait()
    ocean = ocean_of(0, 0)

    chosen[...] = jnp.zeros_like(chosen)
    for q in range(2 * levels):
        for side, (base, top) in enumerate(((0, 0), (LANES - 16, LANES - EDGE))):
            ck, cl = iota((16, LANES), 0) + base, iota((16, LANES), 1)
            hit = (ck >= top) & (ck < top + EDGE) & (ck - top == cl - 2 * nk - EDGE * q)
            chosen[side, pl.ds(q * LANES + base, 16)] = jnp.where(hit, 1.0, 0.0).astype(BF16)
    band_rows[...] = jnp.zeros_like(band_rows)
    for g in range(n_gx):
        band_rows[pl.ds(g * trows, trows), pl.ds(0, srows)] = band_ref[g].astype(F32)
    brows = band_rows.shape[0]
    out_r, in_r = n_gx * lev_rows, lev_grp * cy
    flat = band_rows[...].astype(BF16)
    ri, rq = iota((out_r, brows), 0), iota((out_r, brows), 1)
    pick_r = (lax.div(ri, lev_rows) == lax.div(rq, trows)) & (
        lax.rem(ri, trows) == lax.rem(rq, trows)
    )
    spread = jnp.dot(pick_r.astype(F32).astype(BF16), flat, preferred_element_type=F32)
    cs, cc = iota((LANES, in_r), 0), iota((LANES, in_r), 1)
    pick_c = (lax.rem(lax.rem(cc, cy), srows) == cs).astype(F32).astype(BF16)
    spread = jnp.dot(spread.astype(BF16), pick_c, preferred_element_type=F32)
    ai, ac = iota((out_r, in_r), 0), iota((out_r, in_r), 1)
    keep = (lax.div(lax.rem(ai, lev_rows), trows) == lax.div(ac, cy)) & (
        lax.div(lax.rem(ac, cy), srows) == lax.div(ai, lev_rows)
    )
    band = jnp.where(keep, spread, 0.0).astype(BF16)

    level0 = role * levels

    def stencil(u, v, kap):
        return 1.0 - 4.0 * kap, kap - u, kap + u, kap - v, kap + v

    def advance(c, e, w, n, b, coef):
        own, to_e, to_w, to_n, to_b = coef
        return (own * c + (to_e * e + to_w * w)) + (to_n * n + to_b * b)

    def whole(c, coef):
        tiles_of = range(len(c))
        left = [turn(a, -1, 1) for a in c]
        right = [turn(a, 1, 1) for a in c]
        out = []
        for i in tiles_of:
            e = jnp.where(lane == LANES - 1, left[i + 1], left[i]) if i + 1 < len(c) else left[i]
            w = jnp.where(lane == 0, right[i - 1], right[i]) if i else right[i]
            out.append(advance(c[i], e, w, turn(c[i], -1, 0), turn(c[i], 1, 0), coef[i]))
        return out

    def mean_fields(t1, s1, t2, s2, factor):
        t, s = t1 + t2, s1 + s2
        rho = 0.39 * s - (0.5 * factor) * t - 0.01 * (t1 * t1 + t2 * t2)
        return 0.5 * t, 0.5 * s, rho

    def factor_of(l):
        return 0.17 * (1.0 + 0.03 * (level0 + l).astype(F32))

    flag0 = ocean[:, :LANES]
    half0 = 0.5 * flag0
    wide = iota((1, cx), 1)
    at_edge = (wide < 2) | (wide >= cx - 2)
    tiles = cx // LANES
    order = list(range(n_gx - 1, 0, -1))
    at_end = (gx == 0) | (gx == n_gx - 1)

    def bulk(h, d):
        target = partner(gx, d, n_gx)
        return target, pltpu.make_async_remote_copy(
            src_ref=lat_send.at[h, target],
            dst_ref=lat[h].at[pl.ds(gx * tiles, tiles)],
            send_sem=a2a_send_sems.at[h, d],
            recv_sem=a2a_recv_sems.at[h, d],
            device_id=(role, gy, target),
            device_id_type=MESH,
        )

    def local(h):
        return pltpu.make_async_copy(
            lat_send.at[h, gx],
            lat[h].at[pl.ds(gx * tiles, tiles)],
            local_sems.at[h],
        )

    def stage(h, g, f, rows):
        for i in range(tiles):
            lat_send[h, g, i, pl.ds(f * lev_rows, lev_rows)] = rows[
                :, i * LANES : (i + 1) * LANES
            ]

    def main_levels(first_level, last_level):
        for l in range(first_level, last_level):
            kap = kappa_ref[l] * flag0
            spans = [pl.ds(i * LANES, LANES) for i in range(tiles)]
            coef = [
                stencil(
                    uv[0, l, :, span].astype(F32) * half0, uv[1, l, :, span].astype(F32) * half0, kap
                )
                for span in spans
            ]
            one = [whole([x0[t, l, :, span] for span in spans], coef) for t in range(2)]
            two = [whole(one[t], coef) for t in range(2)]
            factor = factor_of(l)
            for i, span in enumerate(spans):
                x1[0, l, :, span] = one[0][i]
                x1[1, l, :, span] = one[1][i]
                fields = mean_fields(one[0][i], one[1][i], two[0][i], two[1][i], factor)
                for f in range(3):
                    means[f, l, :, span] = fields[f].astype(BF16)

    def main_lat(h):
        for f in range(3):
            rows = means[f, pl.ds(h * lev_grp, lev_grp)].reshape(in_r, cx)
            got = jnp.dot(band[lev_rows : out_r - lev_rows], rows, preferred_element_type=F32)
            got = jnp.where(at_edge, 0.0, got).astype(BF16)
            for g in range(1, n_gx - 1):
                stage(h, g, f, got[(g - 1) * lev_rows : g * lev_rows])

    def held(target):
        return (target == n_gx // 2 - 1) | (target == n_gx // 2)

    def send_half(h):
        for d in order:
            target, copy = bulk(h, d)
            now = (target > 0) & (target < n_gx - 1)
            if h == halves - 1:
                now = now & jnp.logical_not(held(target))
            pl.when(now)(copy.start)
        pl.when(jnp.logical_not(at_end))(local(h).start)

    for load in loads[0]:
        load.wait()
    main_levels(0, SPLIT)
    for later in loads[1:]:
        for load in later:
            load.wait()
    packed = []
    for side, edge in enumerate((pl.ds(0, LANES), pl.ds(cx - LANES, LANES))):
        block = jnp.concatenate(
            [uv[q // levels, q % levels, :, edge] for q in range(2 * levels)], axis=1
        )
        block = jnp.dot(block, chosen[side], preferred_element_type=F32)
        for q in range(2 * levels):
            tile = x0[q // levels, q % levels, :, edge]
            block = jnp.where(quad == q, turn(tile, EDGE * (q + side), 1), block)
        packed.append(block)
    first, last = packed
    cols[1, pl.ds(SUB, cy)] = first
    cols[2, pl.ds(SUB, cy)] = last
    mid = cy // 2

    def fold(block):
        return jnp.where(lane < 2 * nk, block[:mid], turn(block[mid:], 2 * nk, 1))

    fold_send[0] = fold(jnp.where(col < 2, first, turn(first, 2 - 2 * nk, 1)))
    fold_send[1] = fold(jnp.where(col < 2, turn(last, -2 - 2 * nk, 1), last))

    west = wrap(gx + n_gx - 1, n_gx)
    east = wrap(gx + 1, n_gx)
    plan = [
        (None, None, fold_send.at[0], fold_recv.at[0], (role, gy, west)),
        (None, None, fold_send.at[1], fold_recv.at[1], (role, gy, east)),
    ]
    for side, (can_send, can_recv) in enumerate(((has_below, has_above), (has_above, has_below))):
        ty = gy - 1 if side == 0 else gy + 1
        mine = SUB if side == 0 else cy
        theirs = SUB + cy if side == 0 else 0
        for block, there, tx in ((1, 1, gx), (2, 2, gx), (1, 3, west), (2, 0, east)):
            plan.append(
                (
                    can_send,
                    can_recv,
                    cols.at[block, pl.ds(mine, SUB)],
                    cols.at[there, pl.ds(theirs, SUB)],
                    (role, ty, tx),
                )
            )
        row = 0 if side == 0 else cy - 2
        slot = 0 if side == 0 else SUB - 2
        for t, ref in enumerate((temp_hbm, salt_hbm)):
            plan.append(
                (
                    can_send,
                    can_recv,
                    ref.at[:, pl.ds(row, 2), :],
                    halo_x.at[1 - side, t, :, pl.ds(slot, 2), :],
                    (role, ty, gx),
                )
            )
        row = 0 if side == 0 else cy - SUB
        for t, ref in enumerate((zonal_hbm, merid_hbm)):
            plan.append(
                (
                    can_send,
                    can_recv,
                    ref.at[:, pl.ds(row, SUB), :],
                    halo_uv.at[1 - side, t],
                    (role, ty, gx),
                )
            )

    def when(cond, do):
        if cond is None:
            do()
        else:
            pl.when(cond)(do)

    halos = []
    for i, (can_send, can_recv, src, dst, target) in enumerate(plan):
        copy = pltpu.make_async_remote_copy(
            src_ref=src,
            dst_ref=dst,
            send_sem=halo_send_sems.at[i],
            recv_sem=halo_recv_sems.at[i],
            device_id=target,
            device_id_type=MESH,
        )
        halos.append((can_send, can_recv, copy))
    column_halos = halos[:2] + halos[2:6] + halos[10:14]
    row_halos = halos[6:10] + halos[14:18]

    pl.semaphore_wait(barrier, len(greeted))
    for can_send, _, copy in halos:
        when(can_send, copy.start)
    main_levels(SPLIT, lev_grp)
    main_lat(0)
    send_half(0)
    for load in panel_loads:
        load.start()
    for h in range(1, halves):
        main_levels(h * lev_grp, (h + 1) * lev_grp)
        main_lat(h)
        send_half(h)

    cye = cy + 2 * SUB
    row_e = iota((cye, 1), 0)
    kap_l = jnp.zeros((1, LANES), F32)
    factor_l = jnp.zeros((1, LANES), F32)
    lane_level = lax.div(lax.rem(lane, nk), EDGE)
    for l in range(levels):
        kap_l = jnp.where(lane_level == l, kappa_ref[l], kap_l)
        factor_l = jnp.where(lane_level == l, factor_of(l), factor_l)

    flags = {(dy, dx): ocean_of(dy, dx)[:, :LANES] for dy in (-1, 0, 1) for dx in (-1, 0, 1)}

    def coefficients(i, dx):
        block = cols[i]
        oc = jnp.where(
            row_e < SUB, flags[-1, dx], jnp.where(row_e < SUB + cy, flags[0, dx], flags[1, dx])
        )
        half = 0.5 * oc
        u = jnp.where(lane < nk, turn(block, -2 * nk, 1), turn(block, -nk, 1)) * half
        v = jnp.where(lane < nk, turn(block, -3 * nk, 1), turn(block, -2 * nk, 1)) * half
        return stencil(u, v, kap_l * oc)

    def step_left(left, right, coef):
        e = jnp.where(col == EDGE - 1, turn(right, EDGE - 1, 1), turn(left, -1, 1))
        return advance(left, e, turn(left, 1, 1), turn(left, -1, 0), turn(left, 1, 0), coef)

    def step_right(left, right, coef):
        w = jnp.where(col == 0, turn(left, 1 - EDGE, 1), turn(right, 1, 1))
        return advance(right, turn(right, -1, 1), w, turn(right, -1, 0), turn(right, 1, 0), coef)

    for _, can_recv, copy in column_halos:
        when(can_recv, copy.wait_recv)
    for i, (block, shift) in enumerate(((3, 2 * nk - 2), (0, 2 * nk + 2))):
        got = fold_recv[i]
        for part, tail in enumerate((got, turn(got, 2 * nk, 1))):
            cols[block, pl.ds(SUB + part * mid, mid)] = jnp.where(
                lane < 2 * nk, tail, turn(tail, shift, 1)
            )
    own = coefficients(1, 0)
    left1 = step_left(cols[0], cols[1], coefficients(0, -1))
    west1 = step_right(cols[0], cols[1], own)
    west2 = step_right(left1, west1, own)
    own = coefficients(2, 0)
    east1 = step_left(cols[2], cols[3], own)
    right1 = step_right(cols[2], cols[3], coefficients(3, 1))
    east2 = step_left(east1, right1, own)
    both1 = jnp.where(col < 2, west1, east1)[SUB : SUB + cy]
    both2 = jnp.where(col < 2, west2, east2)[SUB : SUB + cy]
    temp_salt, _, rho = mean_fields(
        both1, turn(both1, -nk, 1), both2, turn(both2, -nk, 1), factor_l
    )
    packed = jnp.where(
        lane < 2 * nk, temp_salt, jnp.where(lane < 3 * nk, turn(rho, 2 * nk, 1), 0.0)
    ).astype(BF16)
    narrow = n_gx * trows
    thin = jnp.dot(flat[:narrow], pick_c[:, :cy], preferred_element_type=F32)
    ei, ec = iota((narrow, cy), 0), iota((narrow, cy), 1)
    thin = jnp.where(lax.div(ec, srows) == lax.div(ei, trows), thin, 0.0).astype(BF16)
    edge_lat = jnp.dot(thin, packed, preferred_element_type=F32).astype(BF16)
    for g in range(n_gx):
        e_send[g] = edge_lat[g * trows : (g + 1) * trows]

    e_copies = []
    for d in order:
        target = partner(gx, d, n_gx)
        copy = pltpu.make_async_remote_copy(
            src_ref=e_send.at[target],
            dst_ref=e_recv.at[gx],
            send_sem=e_send_sems.at[d],
            recv_sem=e_recv_sems.at[d],
            device_id=(role, gy, target),
            device_id_type=MESH,
        )
        copy.start()
        e_copies.append(copy)
    e_recv[pl.ds(gx, 1)] = e_send[pl.ds(gx, 1)]

    for _, can_recv, copy in row_halos:
        when(can_recv, copy.wait_recv)
    sub8 = iota((SUB, 1), 0)
    ocean_below, ocean_above = ocean_of(-1, 0), ocean_of(1, 0)

    def up(a, b):
        return jnp.where(sub8 == SUB - 1, turn(b, -1, 0), turn(a, -1, 0))

    def down(a, b):
        return jnp.where(sub8 == 0, turn(a, 1, 0), turn(b, 1, 0))

    def rows_step(c, n, b, coef):
        return advance(c, turn(c, -1, 1), turn(c, 1, 1), n, b, coef)

    for l in range(levels):
        kap = kappa_ref[l] * ocean
        factor = factor_of(l)
        flow = [uv[i, l, pl.ds(0, 16)].astype(F32)[:SUB] * (0.5 * ocean) for i in range(2)]
        other = [halo_uv[0, i, l].astype(F32) * (0.5 * ocean_below) for i in range(2)]
        flow = stencil(*flow, kap)
        other = stencil(*other, kappa_ref[l] * ocean_below)
        ones, twos = [], []
        for t in range(2):
            far, edge, near = halo_x[0, t, l], x0[t, l, pl.ds(0, SUB)], x0[t, l, pl.ds(SUB, SUB)]
            out1 = rows_step(far, up(far, edge), turn(far, 1, 0), other)
            in1 = rows_step(edge, up(edge, near), down(far, edge), flow)
            ones.append(in1)
            next1 = x1[t, l, pl.ds(SUB, SUB)]
            twos.append(rows_step(in1, up(in1, next1), down(out1, in1), flow))
        for f, value in enumerate(mean_fields(*ones, *twos, factor)):
            means[f, l, pl.ds(0, SUB)] = value.astype(BF16)

        flow = [uv[i, l, pl.ds(cy - 16, 16)].astype(F32)[SUB:] * (0.5 * ocean) for i in range(2)]
        other = [halo_uv[1, i, l].astype(F32) * (0.5 * ocean_above) for i in range(2)]
        flow = stencil(*flow, kap)
        other = stencil(*other, kappa_ref[l] * ocean_above)
        ones, twos = [], []
        for t in range(2):
            far = halo_x[1, t, l]
            edge = x0[t, l, pl.ds(cy - SUB, SUB)]
            near = x0[t, l, pl.ds(cy - 2 * SUB, SUB)]
            out1 = rows_step(far, turn(far, -1, 0), down(edge, far), other)
            in1 = rows_step(edge, up(edge, far), down(near, edge), flow)
            ones.append(in1)
            next1 = x1[t, l, pl.ds(cy - 2 * SUB, SUB)]
            twos.append(rows_step(in1, up(in1, out1), down(next1, in1), flow))
        for f, value in enumerate(mean_fields(*ones, *twos, factor)):
            means[f, l, pl.ds(cy - SUB, SUB)] = value.astype(BF16)

    ends = jnp.concatenate([band[:lev_rows], band[out_r - lev_rows :]], axis=0)
    for h in range(halves):
        for f in range(3):
            rows = means[f, pl.ds(h * lev_grp, lev_grp)].reshape(in_r, cx)
            got = jnp.dot(ends, rows, preferred_element_type=F32)
            got = jnp.where(at_edge, 0.0, got).astype(BF16)
            stage(h, 0, f, got[:lev_rows])
            stage(h, n_gx - 1, f, got[lev_rows:])
        pl.when(at_end)(local(h).start)
    for d in order:
        for h in range(halves):
            target, copy = bulk(h, d)
            pl.when((target == 0) | (target == n_gx - 1))(copy.start)

    for d in order:
        target, copy = bulk(halves - 1, d)
        pl.when(held(target))(copy.start)

    depth = sw + LANES
    sub = iota((1, SUB, 1), 1)

    def tile_of(j):
        return lax.div(start_ref[j], LANES)

    blank = jnp.zeros((SUB, tb), F32)
    for j in range(nblk):
        panel_loads[j].wait()
        off = jnp.full((1, tb), start_ref[j] - tile_of(j) * LANES, jnp.int32)
        rows = panel[j].astype(F32)
        parts = [rows[i * SUB : (i + 1) * SUB] for i in range(sw // SUB)]
        bit = 1
        while bit < SUB:
            taken = lax.rem(lax.div(off, bit), 2) == 1
            low = sub8 < bit
            ring = [turn(part, bit, 0) for part in parts] + [blank]
            parts = [
                jnp.where(
                    taken,
                    jnp.where(low, ring[i - 1] if i else blank, ring[i]),
                    parts[i] if i < len(parts) else blank,
                )
                for i in range(len(ring))
            ] if bit == 1 else [
                jnp.where(taken, jnp.where(low, ring[i - 1] if i else blank, ring[i]), parts[i])
                for i in range(len(parts))
            ]
            bit *= 2
        step = 1
        while step * SUB < LANES:
            taken = lax.rem(lax.div(off, step * SUB), 2) == 1
            longer = len(parts) + step
            parts = [
                jnp.where(
                    taken,
                    parts[i - step] if i >= step else blank,
                    parts[i] if i < len(parts) else blank,
                )
                for i in range(longer)
            ]
            step *= 2
        assert len(parts) == depth // SUB
        shifted[j] = jnp.concatenate(parts, axis=0).astype(BF16)

    glanes = gather.shape[2]
    lanes = iota((1, glanes), 1)
    labels = lax.rem(lanes, groups)

    def add_area(r, so_far):
        return so_far + jnp.where(labels == cluster_ref[r], area_ref[r], 0.0)

    area_sum = lax.fori_loop(
        0, cluster_ref.shape[0], add_area, jnp.zeros((1, glanes), F32), unroll=8
    )
    thick_total = sum(1.0 + 0.25 * k for k in range(levels * n_role))
    denom = area_sum * (thick_total * nblk * tb)
    first_row = (gy * n_gx + gx) * trows
    out_rows = halves * half_rows
    orow = iota((out_rows, 1), 0)
    ti = lax.rem(orow, trows)
    hot = jnp.zeros((out_rows, glanes), F32)
    for t in range(trows):
        row_hot = jnp.where(labels == cluster_ref[first_row + t], area_ref[first_row + t], 0.0)
        hot = jnp.where(ti == t, row_hot, hot)
    olevel = lax.div(orow, half_rows) * lev_grp + lax.div(lax.rem(orow, lev_rows), trows)
    ofield = lax.div(lax.rem(orow, half_rows), lev_rows)
    thick = 1.0 + 0.25 * (level0 + olevel).astype(F32)
    field = lax.div(lanes, groups)
    hot = jnp.where(ofield == field, hot * thick, 0.0)

    pk, pc = iota((LANES, cx), 0), iota((LANES, cx), 1)
    place = jnp.where(pc < 2, pc, jnp.where(pc >= cx - 2, pc - (cx - EDGE), -1))
    place = (place == lax.rem(pk, EDGE)).astype(F32).astype(BF16)
    mine_q = ofield * levels + olevel
    for copy in e_copies:
        copy.wait_recv()
    for s in range(n_gx):
        block = e_recv[s].astype(F32)
        tall = jnp.concatenate([block] * (out_rows // trows), axis=0)
        tall = jnp.where(quad == mine_q, tall, 0.0).astype(BF16)
        put = jnp.dot(tall, place, preferred_element_type=F32).astype(BF16)
        for i in range(tiles):
            placed[s * tiles + i] = put[:, i * LANES : (i + 1) * LANES]

    weighted = []
    for h in range(halves):
        for d in order:
            bulk(h, d)[1].wait_recv()
        local(h).wait()
        rows = pl.ds(h * half_rows, half_rows)
        for i in range(n_gx * tiles):
            lat[h][i] = lat[h][i] + placed[i, rows]
        squares = jnp.zeros((half_rows, tb), F32)
        for j in range(nblk):
            tile = tile_of(j)
            window = jnp.concatenate([lat[h][tile + i] for i in range(depth // LANES)], axis=1)
            values = jnp.dot(window, shifted[j], preferred_element_type=F32)
            squares = squares + values * values
            result[rows, pl.ds(j * tb, tb)] = values
        weighted.append(jnp.sum(squares, axis=1, keepdims=True))
    weighted = jnp.concatenate(weighted, axis=0) * hot
    part = jnp.sum(weighted, axis=0, keepdims=True) / denom

    def for_others(do):
        if total <= 64:
            for d in range(1, total):
                do(peer(d))
        else:

            @pl.loop(1, total)
            def _(d):
                do(peer(d))

    def send(device):
        pltpu.make_async_remote_copy(
            src_ref=gather.at[me],
            dst_ref=gather.at[me],
            send_sem=sum_sems.at[0],
            recv_sem=sum_sems.at[1],
            device_id=device,
            device_id_type=MESH,
        ).start()

    gather[me] = part
    for_others(send)

    for h in range(halves):
        for f in range(3):
            for i in range(lev_grp):
                row = h * half_rows + f * lev_rows + i * trows
                out_ref[f, h * lev_grp + i] = result[pl.ds(row, trows), :].astype(BF16)

    for can_send, _, copy in halos:
        when(can_send, copy.wait_send)
    for h in range(halves):
        for d in order:
            bulk(h, d)[1].wait_send()
    for copy in e_copies:
        copy.wait_send()
    every = gather.at[pl.ds(0, total - 1)]
    for i in (1, 0):
        pltpu.make_async_copy(every, every, sum_sems.at[i]).wait()
    sums = jnp.sum(gather[...], axis=0)
    for f in range(3):
        sums_ref[pl.ds(f, 1), :] = turn(sums, -f * groups, 1)[:, :groups]


def store_kernel(remapped_ref, sums_ref, remapped_hbm, sums_hbm, sems):
    copies = [
        pltpu.make_async_copy(remapped_ref, remapped_hbm, sems.at[0]),
        pltpu.make_async_copy(sums_ref, sums_hbm, sems.at[1]),
    ]
    for copy in copies:
        copy.start()
    for copy in copies:
        copy.wait()


def body(
    dims,
    area,
    thermal_anomaly,
    saltiness_anomaly,
    zonal_flow_fraction,
    meridional_flow_fraction,
    mixing_coefficient,
    continent_patch_numbering,
    parallel_band_coefficients,
    meridian_panel_coefficients,
    panel_starting_source_meridian,
    target_parallel_cluster,
):
    n_role, n_gy, n_gx, levels, cy, cx, trows, srows, nblk, sw, tb, groups = dims
    total = n_role * n_gy * n_gx
    lev_grp = 16 // trows
    halves = levels // lev_grp
    half_rows = 3 * lev_grp * trows
    glanes = -(-3 * groups // LANES) * LANES
    hbm = pl.BlockSpec(memory_space=pltpu.MemorySpace.HBM)
    vmem = pl.BlockSpec(memory_space=pltpu.VMEM)
    brows = -(-n_gx * trows // LANES) * LANES
    dma = pltpu.SemaphoreType.DMA
    columns = n_gx * cx
    out_rows = halves * half_rows
    remapped, sums = pl.pallas_call(
        functools.partial(kernel, dims),
        out_shape=(
            jax.ShapeDtypeStruct((3, levels, trows, nblk * tb), BF16),
            jax.ShapeDtypeStruct((3, groups), F32),
        ),
        in_specs=[hbm] * 11,
        out_specs=(vmem, vmem),
        scratch_shapes=[
            pltpu.SMEM(mixing_coefficient.shape, F32),
            pltpu.SMEM(continent_patch_numbering.shape, jnp.int32),
            pltpu.SMEM(panel_starting_source_meridian.shape, jnp.int32),
            pltpu.SMEM(target_parallel_cluster.shape, jnp.int32),
            pltpu.SMEM(area.shape, F32),
            pltpu.VMEM(parallel_band_coefficients.shape, BF16),
            pltpu.VMEM((2, levels, cy, cx), F32),
            pltpu.VMEM((2, levels, cy, cx), F32),
            pltpu.VMEM((2, levels, cy, cx), BF16),
            pltpu.VMEM((3, levels, cy, cx), BF16),
            pltpu.VMEM((2, 2, levels, SUB, cx), F32),
            pltpu.VMEM((2, 2, levels, SUB, cx), BF16),
            pltpu.VMEM((4, cy + 2 * SUB, LANES), F32),
            pltpu.VMEM((2, cy // 2, LANES), F32),
            pltpu.VMEM((2, cy // 2, LANES), F32),
            pltpu.VMEM((2, 2 * levels * LANES, LANES), BF16),
            pltpu.VMEM((brows, LANES), F32),
            pltpu.VMEM((halves, n_gx, cx // LANES, half_rows, LANES), BF16),
            tuple(
                pltpu.VMEM((columns // LANES + 1, half_rows, LANES), BF16) for _ in range(halves)
            ),
            pltpu.VMEM((n_gx, trows, LANES), BF16),
            pltpu.VMEM((n_gx, trows, LANES), BF16),
            pltpu.VMEM((columns // LANES, out_rows, LANES), BF16),
            pltpu.VMEM((nblk, sw, tb), BF16),
            pltpu.VMEM((nblk, sw + LANES, tb), BF16),
            pltpu.VMEM((out_rows, nblk * tb), F32),
            pltpu.VMEM((total, 1, glanes), F32),
            dma((halves, 4)),
            dma((6,)),
            dma((nblk,)),
            dma((18,)),
            dma((18,)),
            dma((halves, n_gx)),
            dma((halves, n_gx)),
            dma((halves,)),
            dma((n_gx,)),
            dma((n_gx,)),
            dma((2,)),
        ],
        compiler_params=pltpu.CompilerParams(
            collective_id=0, has_side_effects=True, vmem_limit_bytes=26 * 1024 * 1024
        ),
        name="ocean",
    )(
        *(
            pltpu.with_memory_space_constraint(array, pltpu.MemorySpace.HBM)
            for array in (
                thermal_anomaly,
                saltiness_anomaly,
                zonal_flow_fraction,
                meridional_flow_fraction,
                meridian_panel_coefficients,
                mixing_coefficient,
                continent_patch_numbering,
                panel_starting_source_meridian,
                target_parallel_cluster,
                jnp.asarray(area),
                parallel_band_coefficients,
            )
        )
    )
    return pl.pallas_call(
        store_kernel,
        out_shape=(
            jax.ShapeDtypeStruct(remapped.shape, BF16),
            jax.ShapeDtypeStruct(sums.shape, F32),
        ),
        in_specs=[vmem, vmem],
        out_specs=(hbm, hbm),
        scratch_shapes=[dma((2,))],
        compiler_params=pltpu.CompilerParams(vmem_limit_bytes=4 * 1024 * 1024),
        name="store",
    )(remapped, sums)


def solution(mesh):
    in_specs = (
        P("role", "gy", "gx"),
        P("role", "gy", "gx"),
        P("role", "gy", "gx"),
        P("role", "gy", "gx"),
        P("role"),
        P(),
        P("gy", None, None),
        P(),
        P(),
        P(),
    )
    out_specs = (P(None, "role", ("gy", "gx"), None), P())

    def run(*args):
        n_role, n_gy, n_gx = (mesh.shape[a] for a in ("role", "gy", "gx"))
        levels, rows, cols = args[0].shape
        _, trows, srows = args[6].shape
        nblk, sw, tb = args[7].shape
        dims = (
            n_role,
            n_gy,
            n_gx,
            levels // n_role,
            rows // n_gy,
            cols // n_gx,
            trows,
            srows,
            nblk,
            sw,
            tb,
            4 * n_gy,
        )
        nrows = args[9].shape[0]
        r = np.arange(nrows, dtype=np.float64)
        area = np.cos((-75.0 + 150.0 * (r + 0.5) / nrows) * (math.pi / 180.0)).astype(np.float32)
        return jax.shard_map(
            functools.partial(body, dims, area),
            mesh=mesh,
            in_specs=in_specs,
            out_specs=out_specs,
            check_vma=False,
        )(*args)

    return run
```
